32 devices in a mesh: seq: 8 (over z, x), kvh: 4 (over y, core).
Axes of the slice: x: 2, y: 2, z: 4, core: 2. Of those that a mesh axis runs over, the one named last changes fastest.
Arguments:
- queries: bfloat16 [1024, 28, 128], P('seq', 'kvh'), may hold values from -80 to 80
- new_keys: bfloat16 [1024, 4, 128], P('seq', 'kvh'), may hold values from -8 to 8
- cache_keys: bfloat16 [512, 4, 128], P('seq', 'kvh'), may hold values from -1.1953125 to 1.1953125
- window_start: int32 [8], replicated, may hold values from 0 to 512, as said below
- owner_slot: int32 [8], replicated, may hold values from 0 to 511, as said below
Outputs:
- relevance: bfloat16 [1024, 28, 512], P('seq', 'kvh')
- rep_bank: bfloat16 [512, 4, 128], P('seq', 'kvh')
The draws below stay inside these ranges and needn't reach their ends.
Inputs may be any that keep to these rules, and one draw needn't show every extreme that they name: `window_start`: each window lies inside the new tokens; some window begins at the first new token and some ends at the last. `owner_slot`: the slots are distinct; the first and the last memory block are always among them.
All inputs are finite; a program needn't handle non-finite values.
Results may differ from the reference program's by a relative error of at most 0.0018.
Values may be sent and summed in bfloat16 or wider, within the bound.
No kernel may reach another device: no remote copies, remote signals or barrier semaphores. Data moves between devices by JAX's collectives and lax.ppermute only.
A program may use at most 64 MiB of HBM per device.

```python
import math
import jax
import jax.numpy as jnp
from jax import lax

HEADS = 28
KVH = 4
HD = 128
BLK = 128
WIN = 512
QTOK = 1024
NEWB = 8
CACHEB = 512


def joint_draw(key):
    key_query = jax.random.fold_in(key, 11)
    key_keys = jax.random.fold_in(key, 12)
    key_window = jax.random.fold_in(key, 13)
    key_ends = jax.random.fold_in(key, 16)
    starts = jax.random.randint(key_window, (NEWB,), 0, QTOK - WIN + 1).astype(jnp.int32)
    end_keys = jax.random.split(key_ends, 2)
    first_pick = jax.random.randint(end_keys[0], (), 0, NEWB).astype(jnp.int32)
    second_pick = ((first_pick + 1 + jax.random.randint(end_keys[1], (), 0, NEWB - 1)) % NEWB).astype(jnp.int32)
    starts = starts.at[first_pick].set(jnp.int32(0))
    starts = starts.at[second_pick].set(jnp.int32(QTOK - WIN))
    key_rows = jnp.clip(jax.random.normal(key_keys, (QTOK, KVH, HD), jnp.float32), -8.0, 8.0)
    query_rows = jnp.clip(jax.random.normal(key_query, (QTOK, HEADS, HD), jnp.float32), -8.0, 8.0)
    return (query_rows, key_rows, starts)


def draw_queries(key, part):
    return joint_draw(key)[0].astype(jnp.bfloat16)


def draw_new_keys(key, part):
    return joint_draw(key)[1].astype(jnp.bfloat16)


def draw_window_start(key, part):
    return joint_draw(key)[2]


def draw_owner_slot(key, part):
    inner = jax.random.permutation(jax.random.fold_in(key, 21), CACHEB - 2)[:NEWB - 2].astype(jnp.int32) + 1
    ends = jnp.array([0, CACHEB - 1], dtype=jnp.int32)
    slots = jnp.concatenate([ends, inner])
    order = jax.random.permutation(jax.random.fold_in(key, 22), NEWB)
    return slots[order].astype(jnp.int32)


def block_scale(key, extent, cuts, low, largest):
    level, own = 1.0, jax.random.fold_in(key, 6)
    for position, shards_of in cuts:
        draws = jnp.exp(jax.random.uniform(jax.random.fold_in(own, position), (shards_of,), jnp.float32, low / len(cuts), largest / len(cuts)))
        level = level * jnp.repeat(draws, extent[position] // shards_of).reshape([-1 if axis == position else 1 for axis in range(len(extent))])
    return level


def normal_values(rng, shape, deviation, reach, pieces=(), held_as=jnp.bfloat16):
    level = block_scale(rng, shape, pieces, -0.22, 0.18) if pieces else 1.0
    values = jax.random.normal(rng, shape, jnp.float32) * deviation * level
    return jnp.minimum(jnp.maximum(values, -reach), reach).astype(held_as)


def setup_inputs(seed: int = 0) -> dict:
    key_list = jax.random.split(jax.random.key(seed), 6)
    queries = draw_queries(jax.random.fold_in(key_list[5], 71), 0)
    new_keys = draw_new_keys(jax.random.fold_in(key_list[5], 71), 0)
    cache_keys = normal_values(key_list[2], (CACHEB, KVH, HD), 0.15, 1.1953125, ((0, 8), (1, 4)))
    window_start = draw_window_start(jax.random.fold_in(key_list[5], 71), 0)
    owner_slot = draw_owner_slot(jax.random.fold_in(key_list[5], 71), 0)
    return {"queries": queries, "new_keys": new_keys, "cache_keys": cache_keys, "window_start": window_start, "owner_slot": owner_slot}


def reference(queries, new_keys, cache_keys, window_start, owner_slot):
    group_size = HEADS // KVH
    score_scale = 1.0 / math.sqrt(HD)

    def one_block(block_index):
        begin = window_start[block_index].astype(jnp.int32)
        window_q = lax.dynamic_slice_in_dim(queries, begin, WIN, 0).astype(jnp.float32)
        window_q = window_q.reshape(WIN, KVH, group_size, HD)
        block_keys = lax.dynamic_slice_in_dim(new_keys, (block_index * BLK).astype(jnp.int32), BLK, 0).astype(jnp.float32)
        scores = jnp.einsum('wgjd,kgd->wgjk', window_q, block_keys, precision=lax.Precision.HIGHEST) * score_scale
        softmax_weights = jax.nn.softmax(scores, axis=-1)
        weights = lax.optimization_barrier(jnp.sum(softmax_weights, axis=(0, 2))) / (group_size * WIN)
        merged = jnp.einsum('gk,kgd->gd', weights, block_keys, precision=lax.Precision.HIGHEST)
        return merged.astype(jnp.bfloat16)
    representative = lax.map(one_block, jnp.arange(NEWB, dtype=jnp.int32))
    key_bank = cache_keys.at[owner_slot].set(representative)
    query_block = math.gcd(QTOK, 512)
    bank_float = key_bank.astype(jnp.float32)

    def score_block(query_part):
        grouped = query_part.astype(jnp.float32).reshape(query_block, KVH, group_size, HD)
        result = jnp.einsum('tgjd,bgd->tgjb', grouped, bank_float) * score_scale
        return result.astype(jnp.bfloat16).reshape(query_block, HEADS, CACHEB)
    relevance = lax.map(score_block, queries.reshape(QTOK // query_block, query_block, HEADS, HD))
    return (relevance.reshape(QTOK, HEADS, CACHEB), key_bank)
```

```python
import functools
import math

import jax
import jax.numpy as jnp
from jax import lax
from jax.experimental import pallas as pl
from jax.experimental.pallas import tpu as pltpu
from jax.sharding import PartitionSpec as P

BLK = 128
WIN = 512
PACK = 16

VMEM = pl.BlockSpec(memory_space=pltpu.VMEM)
SMEM = pl.BlockSpec(memory_space=pltpu.SMEM)


def nt_dot(left, right):
    return lax.dot_general(
        left, right, (((1,), (1,)), ((), ())), preferred_element_type=jnp.float32
    )


def lead_rows(parts):
    return PACK * pl.cdiv(parts, PACK)


def score_kernel(parts, scale, own_ref, mate_ref, mask_ref, *refs):
    key_refs = refs[:parts]
    rep_ref, load_ref = refs[parts:]
    group, tok, _ = own_ref.shape
    bank_rows = key_refs[0].shape[0] - BLK
    here = lax.axis_index("seq") // 2
    lead = lead_rows(parts)
    rep_ref[...] = jnp.zeros_like(rep_ref)
    load_ref[pl.ds(0, lead), :] = jnp.zeros((lead, load_ref.shape[1]), load_ref.dtype)
    for part in range(parts):
        slot = here ^ part
        keys = key_refs[part][pl.ds(0, BLK), :]
        total = jnp.zeros((BLK, tok), jnp.float32)
        for side, query_ref in enumerate((own_ref, mate_ref)):
            inside = mask_ref[side, pl.ds(slot, 1), :]
            for head in range(group):
                scores = nt_dot(keys, query_ref[head])
                top = jnp.max(scores, axis=0, keepdims=True)
                grown = jnp.exp2((scores - top) * scale)
                total += grown * (inside / jnp.sum(grown, axis=0, keepdims=True))
        column = jnp.sum(total, axis=1, keepdims=True)
        rep_ref[pl.ds(slot, 1), :] = jnp.sum(
            column * keys.astype(jnp.float32), axis=0, keepdims=True
        )
        start = pl.multiple_of(lead + slot * bank_rows, PACK)
        load_ref[pl.ds(start, bank_rows), :] = key_refs[part][pl.ds(BLK, bank_rows), :]


def bank_kernel(parts, scale, query_ref, own_ref, mate_ref, slot_ref, rel_ref, bank_ref, work_ref, full_ref):
    rows = bank_ref.shape[0]
    lead = lead_rows(parts)
    me = lax.axis_index("seq")

    @pl.when(pl.program_id(0) == 0)
    def _():
        for side, ref in enumerate((own_ref, mate_ref)):
            lane = (me % 2) ^ side
            for part in range(parts):
                start = pl.multiple_of((2 * part + lane) * rows, rows)
                work_ref[pl.ds(start, rows), :] = ref[pl.ds(lead + part * rows, rows), :].astype(
                    jnp.float32
                )
        for side, ref in enumerate((own_ref, mate_ref)):
            lane = (me % 2) ^ side
            fresh = ref[pl.ds(0, lead), :].astype(jnp.float32)
            for part in range(parts):
                work_ref[pl.ds(slot_ref[2 * part + lane], 1), :] = fresh[part : part + 1]
        full_ref[...] = work_ref[...].astype(jnp.bfloat16)
        bank_ref[...] = full_ref[pl.ds(pl.multiple_of(me * rows, rows), rows), :]

    rel_ref[0] = (nt_dot(query_ref[0], full_ref[...]) * scale).astype(jnp.bfloat16)


def per_device(count, queries, new_keys, cache_keys, window_start, owner_slot):
    tok, group, head_dim = queries.shape
    rows = cache_keys.shape[0]
    parts = count // 2
    assert tok == BLK and count == 1 << (count.bit_length() - 1)
    score_scale = 1.0 / math.sqrt(head_dim)

    def swap(value, mask):
        return lax.ppermute(value, "seq", [(i, i ^ mask) for i in range(count)])

    own = queries.transpose(1, 0, 2)
    mate = swap(own, 1)
    packed = jnp.concatenate([new_keys[:, 0, :], cache_keys[:, 0, :]], axis=0)
    pieces = [packed] + [swap(packed, 2 * k) for k in range(1, parts)]

    me = lax.axis_index("seq")
    sides = jnp.stack([me, me ^ 1])
    position = sides[:, None] * tok + jnp.arange(tok, dtype=jnp.int32)
    starts = window_start.reshape(parts, 2)
    starts = jnp.where(me % 2 == 0, starts[:, 0], starts[:, 1])
    inside = (position[:, None, :] >= starts[None, :, None]) & (
        position[:, None, :] < starts[None, :, None] + WIN
    )
    inside = inside.astype(jnp.float32)

    partial, load = pl.pallas_call(
        functools.partial(score_kernel, parts, score_scale * math.log2(math.e)),
        out_shape=(
            jax.ShapeDtypeStruct((8 * pl.cdiv(parts, 8), head_dim), jnp.float32),
            jax.ShapeDtypeStruct((lead_rows(parts) + parts * rows, head_dim), jnp.bfloat16),
        ),
        in_specs=[VMEM] * (3 + parts),
        out_specs=(VMEM, VMEM),
        name="scores",
    )(own, mate, inside, *pieces)

    step = 2
    while step < count:
        partial = partial + swap(partial, step)
        step *= 2
    fresh = (partial[:parts] * (1.0 / (group * WIN))).astype(jnp.bfloat16)
    load = lax.dynamic_update_slice(load, fresh, (0, 0))
    other = swap(load, 1)

    relevance, bank = pl.pallas_call(
        functools.partial(bank_kernel, parts, score_scale),
        grid=(group,),
        out_shape=(
            jax.ShapeDtypeStruct((group, tok, count * rows), jnp.bfloat16),
            jax.ShapeDtypeStruct((rows, head_dim), jnp.bfloat16),
        ),
        in_specs=[
            pl.BlockSpec((1, tok, head_dim), lambda h: (h, 0, 0)),
            VMEM,
            VMEM,
            SMEM,
        ],
        out_specs=(
            pl.BlockSpec((1, tok, count * rows), lambda h: (h, 0, 0)),
            pl.BlockSpec((rows, head_dim), lambda h: (0, 0)),
        ),
        scratch_shapes=[
            pltpu.VMEM((count * rows, head_dim), jnp.float32),
            pltpu.VMEM((count * rows, head_dim), jnp.bfloat16),
        ],
        name="bank",
    )(own, load, other, owner_slot)
    return (relevance.transpose(1, 0, 2), bank[:, None, :])


def solution(mesh):
    return jax.shard_map(
        functools.partial(per_device, mesh.shape["seq"]),
        mesh=mesh,
        in_specs=(P("seq", "kvh", None), P("seq", "kvh", None), P("seq", "kvh", None), P(), P()),
        out_specs=(P("seq", "kvh", None), P("seq", "kvh", None)),
        check_vma=False,
    )
```

```python
import functools
import math

import jax
import jax.numpy as jnp
from jax import lax
from jax.experimental import pallas as pl
from jax.experimental.pallas import tpu as pltpu
from jax.sharding import PartitionSpec as P

BLK = 128
WIN = 512
PACK = 16
MIB = 1 << 20

VMEM = pl.BlockSpec(memory_space=pltpu.VMEM)
SMEM = pl.BlockSpec(memory_space=pltpu.SMEM)
HBM = pl.BlockSpec(memory_space=pl.ANY)


def nt_dot(left, right):
    return lax.dot_general(
        left, right, (((1,), (1,)), ((), ())), preferred_element_type=jnp.float32
    )


def lead_rows(parts):
    return PACK * pl.cdiv(parts, PACK)


def partial_rep(scale, own_ref, mate_ref, mask_ref, slot, keys):
    group, tok, _ = own_ref.shape
    total = jnp.zeros((BLK, tok), jnp.float32)
    for side, query_ref in enumerate((own_ref, mate_ref)):
        inside = mask_ref[side, pl.ds(slot, 1), :]
        for head in range(group):
            scores = nt_dot(keys, query_ref[head])
            top = jnp.max(scores, axis=0, keepdims=True)
            grown = jnp.exp2((scores - top) * scale)
            total += grown * (inside / jnp.sum(grown, axis=0, keepdims=True))
    column = jnp.sum(total, axis=1, keepdims=True)
    return jnp.sum(column * keys.astype(jnp.float32), axis=0, keepdims=True)


def early_kernel(parts, ahead, scale, start_ref, slot_ref, own_ref, mate_ref, *refs):
    key_refs = refs[:ahead]
    rep_ref, mask_ref, pick_ref = refs[ahead:]
    tok = own_ref.shape[1]
    me = lax.axis_index("seq")
    here, lane = me // 2, me % 2
    lead = lead_rows(parts)
    token = lax.broadcasted_iota(jnp.int32, (1, tok), 1)
    column = lax.broadcasted_iota(jnp.int32, (1, 2 * lead), 1)
    slots = jnp.full((1, 2 * lead), -1, jnp.int32)
    for part in range(parts):
        for side in range(2):
            where = (me ^ side) * tok + token - start_ref[2 * part + lane]
            mask_ref[side, pl.ds(part, 1), :] = ((where >= 0) & (where < WIN)).astype(jnp.float32)
            slots = jnp.where(
                column == side * lead + part, slot_ref[2 * part + (lane ^ side)], slots
            )
    row = lax.broadcasted_iota(jnp.int32, pick_ref.shape, 0)
    pick_ref[...] = (row == slots).astype(jnp.float32).astype(jnp.bfloat16)
    rep_ref[...] = jnp.zeros_like(rep_ref)
    for part in range(ahead):
        slot = here ^ part
        rep_ref[pl.ds(slot, 1), :] = partial_rep(
            scale, own_ref, mate_ref, mask_ref, slot, key_refs[part][pl.ds(0, BLK), :]
        )


def late_kernel(parts, ahead, scale, own_ref, mate_ref, mask_ref, early_ref, *refs):
    key_refs, rep_ref = refs[:-1], refs[-1]
    here = lax.axis_index("seq") // 2
    rep_ref[...] = early_ref[...]
    for part in range(ahead, parts):
        slot = here ^ part
        rep_ref[pl.ds(slot, 1), :] = partial_rep(
            scale, own_ref, mate_ref, mask_ref, slot, key_refs[part - ahead][pl.ds(0, BLK), :]
        )


def load_kernel(parts, share, *refs):
    rep_refs, key_refs, load_ref = refs[:parts], refs[parts:-1], refs[-1]
    rows = key_refs[0].shape[0] - BLK
    here = lax.axis_index("seq") // 2
    lead = lead_rows(parts)
    sums = [ref[...] for ref in rep_refs]
    while len(sums) > 1:
        sums = [left + right for left, right in zip(sums[::2], sums[1::2])]
    load_ref[pl.ds(0, lead), :] = (sums[0] * share).astype(jnp.bfloat16)
    for part in range(parts):
        start = pl.multiple_of(lead + (here ^ part) * rows, PACK)
        load_ref[pl.ds(start, rows), :] = key_refs[part][pl.ds(BLK, rows), :]


def bank_kernel(parts, scale, query_ref, own_ref, mate_ref, pick_ref, rel_ref, bank_ref, base_ref, rel_work, bank_work, sems):
    group = query_ref.shape[0]
    rows = bank_ref.shape[0]
    lead = lead_rows(parts)
    me = lax.axis_index("seq")
    for side, ref in enumerate((own_ref, mate_ref)):
        lane = (me % 2) ^ side
        for part in range(parts):
            start = pl.multiple_of((2 * part + lane) * rows, PACK)
            base_ref[pl.ds(start, rows), :] = ref[pl.ds(lead + part * rows, rows), :]
    fresh = jnp.concatenate([own_ref[pl.ds(0, lead), :], mate_ref[pl.ds(0, lead), :]], axis=0)
    pick = pick_ref[...]
    placed = jnp.dot(pick, fresh, preferred_element_type=jnp.float32)
    taken = jnp.dot(pick, jnp.ones_like(fresh), preferred_element_type=jnp.float32)
    bank = jnp.where(taken > 0.5, placed, base_ref[...].astype(jnp.float32)).astype(jnp.bfloat16)
    base_ref[...] = bank
    bank_work[...] = base_ref[pl.ds(pl.multiple_of(me * rows, PACK), rows), :]
    copies = [pltpu.make_async_copy(bank_work, bank_ref, sems.at[group])]
    copies[0].start()
    for head in range(group):
        rel_work[head] = (nt_dot(query_ref[head], bank) * scale).astype(jnp.bfloat16)
        copies.append(pltpu.make_async_copy(rel_work.at[head], rel_ref.at[head], sems.at[head]))
        copies[-1].start()
    for copy in copies:
        copy.wait()


def per_device(count, queries, new_keys, cache_keys, window_start, owner_slot):
    tok, group, head_dim = queries.shape
    rows = cache_keys.shape[0]
    parts = count // 2
    ahead = max(parts - 1, 1)
    lead = lead_rows(parts)
    assert tok == BLK and count == 1 << (count.bit_length() - 1)
    score_scale = 1.0 / math.sqrt(head_dim)
    exp_scale = score_scale * math.log2(math.e)

    def swap(value, mask):
        return lax.ppermute(value, "seq", [(i, i ^ mask) for i in range(count)])

    def params(mib):
        return pltpu.CompilerParams(vmem_limit_bytes=mib * MIB)

    own = queries.transpose(1, 0, 2)
    mate = swap(own, 1)
    packed = jnp.concatenate([new_keys[:, 0, :], cache_keys[:, 0, :]], axis=0)
    pieces = [packed] + [swap(packed, 2 * k) for k in range(1, parts)]

    sums = jax.ShapeDtypeStruct((lead, head_dim), jnp.float32)
    small = 8 + parts // 2
    partial, inside, pick = pl.pallas_call(
        functools.partial(early_kernel, parts, ahead, exp_scale),
        out_shape=(
            sums,
            jax.ShapeDtypeStruct((2, parts, tok), jnp.float32),
            jax.ShapeDtypeStruct((count * rows, 2 * lead), jnp.bfloat16),
        ),
        in_specs=[SMEM, SMEM] + [VMEM] * (2 + ahead),
        out_specs=(VMEM, VMEM, VMEM),
        compiler_params=params(small),
        name="early",
    )(window_start, owner_slot, own, mate, *pieces[:ahead])
    partial = pl.pallas_call(
        functools.partial(late_kernel, parts, ahead, exp_scale),
        out_shape=sums,
        in_specs=[VMEM] * (4 + parts - ahead),
        out_specs=VMEM,
        compiler_params=params(small),
        name="late",
    )(own, mate, inside, partial, *pieces[ahead:])

    load = pl.pallas_call(
        functools.partial(load_kernel, parts, 1.0 / (group * WIN)),
        out_shape=jax.ShapeDtypeStruct((lead + parts * rows, head_dim), jnp.bfloat16),
        in_specs=[VMEM] * (2 * parts),
        out_specs=VMEM,
        compiler_params=params(small),
        name="load",
    )(partial, *[swap(partial, 2 * k) for k in range(1, parts)], *pieces)
    other = swap(load, 1)

    relevance, bank = pl.pallas_call(
        functools.partial(bank_kernel, parts, score_scale),
        out_shape=(
            jax.ShapeDtypeStruct((group, tok, count * rows), jnp.bfloat16),
            jax.ShapeDtypeStruct((rows, head_dim), jnp.bfloat16),
        ),
        in_specs=[VMEM] * 4,
        out_specs=(HBM, HBM),
        scratch_shapes=[
            pltpu.VMEM((count * rows, head_dim), jnp.bfloat16),
            pltpu.VMEM((group, tok, count * rows), jnp.bfloat16),
            pltpu.VMEM((rows, head_dim), jnp.bfloat16),
            pltpu.SemaphoreType.DMA((group + 1,)),
        ],
        compiler_params=params(8 + parts),
        name="bank",
    )(own, load, other, pick)
    return (relevance.transpose(1, 0, 2), bank[:, None, :])


def solution(mesh):
    return jax.shard_map(
        functools.partial(per_device, mesh.shape["seq"]),
        mesh=mesh,
        in_specs=(P("seq", "kvh", None), P("seq", "kvh", None), P("seq", "kvh", None), P(), P()),
        out_specs=(P("seq", "kvh", None), P("seq", "kvh", None)),
        check_vma=False,
    )
```

```python
import functools
import math

import jax
import jax.numpy as jnp
from jax import lax
from jax.experimental import pallas as pl
from jax.experimental.pallas import tpu as pltpu
from jax.sharding import PartitionSpec as P

BLK = 128
WIN = 512
PACK = 16
MIB = 1 << 20

VMEM = pl.BlockSpec(memory_space=pltpu.VMEM)
SMEM = pl.BlockSpec(memory_space=pltpu.SMEM)
HBM = pl.BlockSpec(memory_space=pltpu.HBM)


def nt_dot(left, right):
    return lax.dot_general(
        left, right, (((1,), (1,)), ((), ())), preferred_element_type=jnp.float32
    )


def padded(rows, unit):
    return unit * pl.cdiv(rows, unit)


def lead_rows(parts):
    return padded(parts, PACK)


def term_rows(parts):
    return padded(3 * parts, PACK)


def column_sums(scale, query_ref, inside, keys):
    group, tok, _ = query_ref.shape

    def one_head(head, total):
        scores = nt_dot(keys, query_ref[head])
        top = jnp.max(scores, axis=0, keepdims=True)
        grown = jnp.exp2((scores - top) * scale)
        return total + grown * (inside / jnp.sum(grown, axis=0, keepdims=True))

    total = jnp.zeros((BLK, tok), jnp.float32)
    return lax.fori_loop(0, group, one_head, total, unroll=True)


def partial_rep(scale, query_refs, mask_refs, keys):
    total = 0.0
    for query_ref, inside in zip(query_refs, mask_refs):
        total += column_sums(scale, query_ref, inside, keys)
    column = jnp.sum(total, axis=1, keepdims=True)
    return jnp.sum(column * keys.astype(jnp.float32), axis=0, keepdims=True)


def first_kernel(parts, scale, start_ref, slot_ref, query_hbm, key_hbm, rep_ref, mask_ref, pick_ref, query_ref, key_ref, sems):
    tok = query_ref.shape[1]
    copies = [
        pltpu.make_async_copy(key_hbm, key_ref, sems.at[0]),
        pltpu.make_async_copy(query_hbm, query_ref, sems.at[1]),
    ]
    for copy in copies:
        copy.start()
    me = lax.axis_index("seq")
    here, lane = me // 2, me % 2
    lead = lead_rows(parts)
    token = lax.broadcasted_iota(jnp.int32, (1, tok), 1)
    column = lax.broadcasted_iota(jnp.int32, (1, 2 * lead), 1)
    slots = jnp.full((1, 2 * lead), -1, jnp.int32)
    for part in range(parts):
        for side in range(2):
            where = (me ^ side) * tok + token - start_ref[2 * part + lane]
            mask_ref[side, pl.ds(part, 1), :] = ((where >= 0) & (where < WIN)).astype(jnp.float32)
            slots = jnp.where(
                column == side * lead + part, slot_ref[2 * part + (lane ^ side)], slots
            )
    row = lax.broadcasted_iota(jnp.int32, pick_ref.shape, 0)
    pick_ref[...] = (row == slots).astype(jnp.float32).astype(jnp.bfloat16)
    rep_ref[...] = jnp.zeros_like(rep_ref)
    for copy in copies:
        copy.wait()
    inside = mask_ref[0, pl.ds(here, 1), :]
    rep_ref[pl.ds(here, 1), :] = partial_rep(scale, [query_ref], [inside], key_ref[...])


def step_kernel(sides, members, scale, mask_ref, prior_ref, *refs):
    query_refs, key_refs, rep_ref = refs[: len(sides)], refs[len(sides) : -1], refs[-1]
    here = lax.axis_index("seq") // 2
    rep_ref[...] = prior_ref[...]
    for part, key_ref in zip(members, key_refs):
        slot = here ^ part
        inside = [mask_ref[side, pl.ds(slot, 1), :] for side in sides]
        rep_ref[pl.ds(slot, 1), :] += partial_rep(scale, query_refs, inside, key_ref[...])


def last_kernel(parts, scale, mask_ref, prior_ref, own_ref, mate_ref, key_ref, cache_ref, sum_ref, rep_ref):
    slot = (lax.axis_index("seq") // 2) ^ (parts - 1)
    rep_ref[...] = prior_ref[...]
    inside = [mask_ref[side, pl.ds(slot, 1), :] for side in range(2)]
    rep_ref[pl.ds(slot, 1), :] += partial_rep(scale, [own_ref, mate_ref], inside, key_ref[...])
    rest = rep_ref[pl.ds(0, parts), :]
    terms = []
    for _ in range(3):
        terms.append(rest.astype(jnp.bfloat16).astype(jnp.float32))
        rest = rest - terms[-1]
    spare = term_rows(parts) - 3 * parts
    if spare:
        terms.append(jnp.zeros((spare, rest.shape[1]), jnp.float32))
    sum_ref[pl.ds(0, term_rows(parts)), :] = jnp.concatenate(terms, axis=0).astype(jnp.bfloat16)
    sum_ref[pl.ds(term_rows(parts), cache_ref.shape[0]), :] = cache_ref[...]


def load_kernel(parts, share, *refs):
    sum_refs, load_ref = refs[:-1], refs[-1]
    terms = term_rows(parts)
    rows = sum_refs[0].shape[0] - terms
    here = lax.axis_index("seq") // 2
    lead = lead_rows(parts)
    sums = []
    for ref in sum_refs:
        wide = ref[pl.ds(0, terms), :].astype(jnp.float32)
        sums.append(wide[:parts] + (wide[parts : 2 * parts] + wide[2 * parts : 3 * parts]))
    while len(sums) > 1:
        sums = [left + right for left, right in zip(sums[::2], sums[1::2])]
    fresh = [sums[0] * share]
    if lead > parts:
        fresh.append(jnp.zeros((lead - parts, fresh[0].shape[1]), jnp.float32))
    load_ref[pl.ds(0, lead), :] = jnp.concatenate(fresh, axis=0).astype(jnp.bfloat16)
    for part in range(parts):
        start = pl.multiple_of(lead + (here ^ part) * rows, PACK)
        load_ref[pl.ds(start, rows), :] = sum_refs[part][pl.ds(terms, rows), :]


def bank_kernel(parts, scale, query_ref, own_ref, mate_ref, pick_ref, rel_ref, bank_ref, base_ref, rel_work, bank_work, sems):
    group = query_ref.shape[0]
    rows = bank_ref.shape[0]
    lead = lead_rows(parts)
    me = lax.axis_index("seq")
    for side, ref in enumerate((own_ref, mate_ref)):
        lane = (me % 2) ^ side
        for part in range(parts):
            start = pl.multiple_of((2 * part + lane) * rows, PACK)
            base_ref[pl.ds(start, rows), :] = ref[pl.ds(lead + part * rows, rows), :]
    fresh = jnp.concatenate([own_ref[pl.ds(0, lead), :], mate_ref[pl.ds(0, lead), :]], axis=0)
    pick = pick_ref[...]
    placed = jnp.dot(pick, fresh, preferred_element_type=jnp.float32)
    taken = jnp.dot(pick, jnp.ones_like(fresh), preferred_element_type=jnp.float32)
    bank = jnp.where(taken > 0.5, placed, base_ref[...].astype(jnp.float32)).astype(jnp.bfloat16)
    base_ref[...] = bank
    bank_work[...] = base_ref[pl.ds(pl.multiple_of(me * rows, PACK), rows), :]
    copies = [pltpu.make_async_copy(bank_work, bank_ref, sems.at[group])]
    copies[0].start()
    for head in range(group):
        rel_work[head] = (nt_dot(query_ref[head], bank) * scale).astype(jnp.bfloat16)
        copies.append(pltpu.make_async_copy(rel_work.at[head], rel_ref.at[head], sems.at[head]))
        copies[-1].start()
    for copy in copies:
        copy.wait()


def per_device(count, queries, new_keys, cache_keys, window_start, owner_slot):
    tok, group, head_dim = queries.shape
    rows = cache_keys.shape[0]
    parts = count // 2
    lead = lead_rows(parts)
    assert tok == BLK and count == 1 << (count.bit_length() - 1) and count > 2
    score_scale = 1.0 / math.sqrt(head_dim)
    exp_scale = score_scale * math.log2(math.e)

    def swap(value, mask):
        return lax.ppermute(value, "seq", [(i, i ^ mask) for i in range(count)])

    def shape(rows_of, dtype):
        return jax.ShapeDtypeStruct((rows_of, head_dim), dtype)

    params = pltpu.CompilerParams(vmem_limit_bytes=(8 + parts) * MIB)
    asked = queries.transpose(1, 0, 2)
    mate = swap(asked, 1)
    keys = new_keys[:, 0, :]
    pieces = [keys] + [swap(keys, 2 * k) for k in range(1, parts)]

    sums = shape(padded(parts, 8), jnp.float32)
    partial, inside, pick, own, held = pl.pallas_call(
        functools.partial(first_kernel, parts, exp_scale),
        out_shape=(
            sums,
            jax.ShapeDtypeStruct((2, parts, tok), jnp.float32),
            jax.ShapeDtypeStruct((count * rows, 2 * lead), jnp.bfloat16),
            jax.ShapeDtypeStruct(asked.shape, jnp.bfloat16),
            jax.ShapeDtypeStruct(keys.shape, jnp.bfloat16),
        ),
        in_specs=[SMEM, SMEM, HBM, HBM],
        out_specs=(VMEM,) * 5,
        scratch_shapes=[pltpu.SemaphoreType.DMA((2,))],
        compiler_params=params,
        name="first",
    )(window_start, owner_slot, asked, keys)
    pieces[0] = held

    def step(partial, sides, members, label):
        asking = [(own, mate)[side] for side in sides]
        return pl.pallas_call(
            functools.partial(step_kernel, sides, members, exp_scale),
            out_shape=sums,
            in_specs=[VMEM] * (2 + len(sides) + len(members)),
            out_specs=VMEM,
            compiler_params=params,
            name=label,
        )(inside, partial, *asking, *[pieces[part] for part in members])

    for part in reversed(range(1, parts - 1)):
        partial = step(partial, (0,), (part,), "own_step")
    partial = step(partial, (1,), tuple(range(parts - 1)), "mate_step")
    partial = pl.pallas_call(
        functools.partial(last_kernel, parts, exp_scale),
        out_shape=shape(term_rows(parts) + rows, jnp.bfloat16),
        in_specs=[VMEM] * 6,
        out_specs=VMEM,
        scratch_shapes=[pltpu.VMEM(sums.shape, sums.dtype)],
        compiler_params=params,
        name="last",
    )(inside, partial, own, mate, pieces[-1], cache_keys[:, 0, :])

    load = pl.pallas_call(
        functools.partial(load_kernel, parts, 1.0 / (group * WIN)),
        out_shape=shape(lead + parts * rows, jnp.bfloat16),
        in_specs=[VMEM] * parts,
        out_specs=VMEM,
        compiler_params=params,
        name="load",
    )(partial, *[swap(partial, 2 * k) for k in range(1, parts)])
    other = swap(load, 1)

    relevance, bank = pl.pallas_call(
        functools.partial(bank_kernel, parts, score_scale),
        out_shape=(
            jax.ShapeDtypeStruct((group, tok, count * rows), jnp.bfloat16),
            jax.ShapeDtypeStruct((rows, head_dim), jnp.bfloat16),
        ),
        in_specs=[VMEM] * 4,
        out_specs=(HBM, HBM),
        scratch_shapes=[
            pltpu.VMEM((count * rows, head_dim), jnp.bfloat16),
            pltpu.VMEM((group, tok, count * rows), jnp.bfloat16),
            pltpu.VMEM((rows, head_dim), jnp.bfloat16),
            pltpu.SemaphoreType.DMA((group + 1,)),
        ],
        compiler_params=params,
        name="bank",
    )(own, load, other, pick)
    return (relevance.transpose(1, 0, 2), bank[:, None, :])


def solution(mesh):
    return jax.shard_map(
        functools.partial(per_device, mesh.shape["seq"]),
        mesh=mesh,
        in_specs=(P("seq", "kvh", None), P("seq", "kvh", None), P("seq", "kvh", None), P(), P()),
        out_specs=(P("seq", "kvh", None), P("seq", "kvh", None)),
        check_vma=False,
    )
```

```python
import functools
import math

import jax
import jax.numpy as jnp
from jax import lax
from jax.experimental import pallas as pl
from jax.experimental.pallas import tpu as pltpu
from jax.sharding import PartitionSpec as P

BLK = 128
WIN = 512
PACK = 16
MIB = 1 << 20

VMEM = pl.BlockSpec(memory_space=pltpu.VMEM)
HBM = pl.BlockSpec(memory_space=pltpu.HBM)


def nt_dot(left, right):
    return lax.dot_general(
        left, right, (((1,), (1,)), ((), ())), preferred_element_type=jnp.float32
    )


def padded(rows, unit):
    return unit * pl.cdiv(rows, unit)


def lead_rows(parts):
    return padded(parts, PACK)


def term_rows(parts):
    return padded(3 * parts, PACK)


def column_sums(scale, query_ref, keys):
    group, tok, _ = query_ref.shape

    def one_head(head, total):
        scores = nt_dot(keys, query_ref[head])
        top = jnp.max(scores, axis=0, keepdims=True)
        grown = jnp.exp2((scores - top) * scale)
        return total + grown * (1.0 / jnp.sum(grown, axis=0, keepdims=True))

    total = jnp.zeros((BLK, tok), jnp.float32)
    return lax.fori_loop(0, group, one_head, total, unroll=True)


def partial_rep(scale, query_refs, insides, keys):
    total = 0.0
    for query_ref, inside in zip(query_refs, insides):
        total += column_sums(scale, query_ref, keys) * inside
    column = jnp.sum(total, axis=1, keepdims=True)
    return jnp.sum(column * keys.astype(jnp.float32), axis=0, keepdims=True)


def first_kernel(
    parts, scale, start_hbm, slot_hbm, query_hbm, key_hbm,
    rep_ref, mask_ref, pick_ref, query_ref, key_ref, start_ref, slot_ref, sems,
):
    pairs = ((start_hbm, start_ref), (slot_hbm, slot_ref), (key_hbm, key_ref), (query_hbm, query_ref))
    copies = [pltpu.make_async_copy(*pair, sems.at[i]) for i, pair in enumerate(pairs)]
    for copy in copies:
        copy.start()
    tok = query_ref.shape[1]
    me = lax.axis_index("seq")
    here, lane = me // 2, me % 2
    lead = lead_rows(parts)
    token = lax.broadcasted_iota(jnp.int32, (1, tok), 1)
    column = lax.broadcasted_iota(jnp.int32, (1, 2 * lead), 1)
    slots = jnp.full((1, 2 * lead), -1, jnp.int32)
    for copy in copies[:2]:
        copy.wait()
    for part in range(parts):
        for side in range(2):
            where = (me ^ side) * tok + token - start_ref[2 * part + lane]
            mask_ref[side, pl.ds(part, 1), :] = ((where >= 0) & (where < WIN)).astype(jnp.float32)
            slots = jnp.where(
                column == side * lead + part, slot_ref[2 * part + (lane ^ side)], slots
            )
    row = lax.broadcasted_iota(jnp.int32, pick_ref.shape, 0)
    pick_ref[...] = (row == slots).astype(jnp.float32).astype(jnp.bfloat16)
    rep_ref[...] = jnp.zeros_like(rep_ref)
    for copy in copies[2:]:
        copy.wait()
    inside = mask_ref[0, pl.ds(here, 1), :]
    rep_ref[pl.ds(here, 1), :] = partial_rep(scale, [query_ref], [inside], key_ref[...])


def step_kernel(sides, members, scale, mask_ref, prior_ref, *refs):
    query_refs, key_refs, rep_ref = refs[: len(sides)], refs[len(sides) : -1], refs[-1]
    here = lax.axis_index("seq") // 2
    rep_ref[...] = prior_ref[...]
    for part, key_ref in zip(members, key_refs):
        slot = here ^ part
        inside = [mask_ref[side, pl.ds(slot, 1), :] for side in sides]
        rep_ref[pl.ds(slot, 1), :] += partial_rep(scale, query_refs, inside, key_ref[...])


def last_kernel(
    parts, part, scale, mask_ref, prior_ref, own_ref, mate_ref, key_ref, cache_ref, sum_ref, rep_ref
):
    slot = (lax.axis_index("seq") // 2) ^ part
    rep_ref[...] = prior_ref[...]
    inside = [mask_ref[side, pl.ds(slot, 1), :] for side in range(2)]
    rep_ref[pl.ds(slot, 1), :] += partial_rep(scale, [own_ref, mate_ref], inside, key_ref[...])
    rest = rep_ref[pl.ds(0, parts), :]
    terms = []
    for _ in range(3):
        terms.append(rest.astype(jnp.bfloat16).astype(jnp.float32))
        rest = rest - terms[-1]
    spare = term_rows(parts) - 3 * parts
    if spare:
        terms.append(jnp.zeros((spare, rest.shape[1]), jnp.float32))
    sum_ref[pl.ds(0, term_rows(parts)), :] = jnp.concatenate(terms, axis=0).astype(jnp.bfloat16)
    sum_ref[pl.ds(term_rows(parts), cache_ref.shape[0]), :] = cache_ref[...]


def load_kernel(parts, share, *refs):
    sum_refs, load_ref = refs[:-1], refs[-1]
    terms = term_rows(parts)
    rows = sum_refs[0].shape[0] - terms
    here = lax.axis_index("seq") // 2
    lead = lead_rows(parts)
    sums = []
    for ref in sum_refs:
        wide = ref[pl.ds(0, terms), :].astype(jnp.float32)
        sums.append(wide[:parts] + (wide[parts : 2 * parts] + wide[2 * parts : 3 * parts]))
    while len(sums) > 1:
        sums = [left + right for left, right in zip(sums[::2], sums[1::2])]
    fresh = [sums[0] * share]
    if lead > parts:
        fresh.append(jnp.zeros((lead - parts, fresh[0].shape[1]), jnp.float32))
    load_ref[pl.ds(0, lead), :] = jnp.concatenate(fresh, axis=0).astype(jnp.bfloat16)
    for part in range(parts):
        start = pl.multiple_of(lead + (here ^ part) * rows, PACK)
        load_ref[pl.ds(start, rows), :] = sum_refs[part][pl.ds(terms, rows), :]


def bank_kernel(parts, scale, query_ref, own_ref, mate_ref, pick_ref, rel_ref, bank_ref, base_ref, rel_work, bank_work, sems):
    group = query_ref.shape[0]
    rows = bank_ref.shape[0]
    lead = lead_rows(parts)
    me = lax.axis_index("seq")
    for side, ref in enumerate((own_ref, mate_ref)):
        lane = (me % 2) ^ side
        for part in range(parts):
            start = pl.multiple_of((2 * part + lane) * rows, PACK)
            base_ref[pl.ds(start, rows), :] = ref[pl.ds(lead + part * rows, rows), :]
    fresh = jnp.concatenate([own_ref[pl.ds(0, lead), :], mate_ref[pl.ds(0, lead), :]], axis=0)
    pick = pick_ref[...]
    placed = jnp.dot(pick, fresh, preferred_element_type=jnp.float32)
    taken = jnp.dot(pick, jnp.ones_like(fresh), preferred_element_type=jnp.float32)
    bank = jnp.where(taken > 0.5, placed, base_ref[...].astype(jnp.float32)).astype(jnp.bfloat16)
    base_ref[...] = bank
    bank_work[...] = base_ref[pl.ds(pl.multiple_of(me * rows, PACK), rows), :]
    copies = [pltpu.make_async_copy(bank_work, bank_ref, sems.at[group])]
    copies[0].start()
    for head in range(group):
        rel_work[head] = (nt_dot(query_ref[head], bank) * scale).astype(jnp.bfloat16)
        copies.append(pltpu.make_async_copy(rel_work.at[head], rel_ref.at[head], sems.at[head]))
        copies[-1].start()
    for copy in copies:
        copy.wait()


def per_device(count, queries, new_keys, cache_keys, window_start, owner_slot):
    tok, group, head_dim = queries.shape
    rows = cache_keys.shape[0]
    parts = count // 2
    lead = lead_rows(parts)
    assert tok == BLK and count == 1 << (count.bit_length() - 1) and count > 2
    score_scale = 1.0 / math.sqrt(head_dim)
    exp_scale = score_scale * math.log2(math.e)

    def swap(value, mask):
        return lax.ppermute(value, "seq", [(i, i ^ mask) for i in range(count)])

    def shape(rows_of, dtype):
        return jax.ShapeDtypeStruct((rows_of, head_dim), dtype)

    params = pltpu.CompilerParams(vmem_limit_bytes=(8 + parts) * MIB)
    asked = queries.transpose(1, 0, 2)
    mate = swap(asked, 1)
    keys = new_keys[:, 0, :]
    pieces = [keys] + [swap(keys, 2 * k) for k in range(1, parts)]

    sums = shape(padded(parts, 8), jnp.float32)
    partial, inside, pick, own, held = pl.pallas_call(
        functools.partial(first_kernel, parts, exp_scale),
        out_shape=(
            sums,
            jax.ShapeDtypeStruct((2, parts, tok), jnp.float32),
            jax.ShapeDtypeStruct((count * rows, 2 * lead), jnp.bfloat16),
            jax.ShapeDtypeStruct(asked.shape, jnp.bfloat16),
            jax.ShapeDtypeStruct(keys.shape, jnp.bfloat16),
        ),
        in_specs=[HBM] * 4,
        out_specs=(VMEM,) * 5,
        scratch_shapes=[
            pltpu.SMEM(window_start.shape, jnp.int32),
            pltpu.SMEM(owner_slot.shape, jnp.int32),
            pltpu.SemaphoreType.DMA((4,)),
        ],
        compiler_params=params,
        name="first",
    )(*[pltpu.with_memory_space_constraint(x, pltpu.HBM) for x in (window_start, owner_slot, asked, keys)])
    pieces[0] = held

    def step(partial, sides, members, label):
        asking = [(own, mate)[side] for side in sides]
        return pl.pallas_call(
            functools.partial(step_kernel, sides, members, exp_scale),
            out_shape=sums,
            in_specs=[VMEM] * (2 + len(sides) + len(members)),
            out_specs=VMEM,
            compiler_params=params,
            name=label,
        )(inside, partial, *asking, *[pieces[part] for part in members])

    *middle, tail = reversed(range(1, parts))
    for part in middle:
        partial = step(partial, (0,), (part,), "own_step")
    partial = step(partial, (1,), (0, *middle), "mate_step")
    partial = pl.pallas_call(
        functools.partial(last_kernel, parts, tail, exp_scale),
        out_shape=shape(term_rows(parts) + rows, jnp.bfloat16),
        in_specs=[VMEM] * 6,
        out_specs=VMEM,
        scratch_shapes=[pltpu.VMEM(sums.shape, sums.dtype)],
        compiler_params=params,
        name="last",
    )(inside, partial, own, mate, pieces[tail], cache_keys[:, 0, :])

    load = pl.pallas_call(
        functools.partial(load_kernel, parts, 1.0 / (group * WIN)),
        out_shape=shape(lead + parts * rows, jnp.bfloat16),
        in_specs=[VMEM] * parts,
        out_specs=VMEM,
        compiler_params=params,
        name="load",
    )(partial, *[swap(partial, 2 * k) for k in range(1, parts)])
    other = swap(load, 1)

    relevance, bank = pl.pallas_call(
        functools.partial(bank_kernel, parts, score_scale),
        out_shape=(
            jax.ShapeDtypeStruct((group, tok, count * rows), jnp.bfloat16),
            jax.ShapeDtypeStruct((rows, head_dim), jnp.bfloat16),
        ),
        in_specs=[VMEM] * 4,
        out_specs=(HBM, HBM),
        scratch_shapes=[
            pltpu.VMEM((count * rows, head_dim), jnp.bfloat16),
            pltpu.VMEM((group, tok, count * rows), jnp.bfloat16),
            pltpu.VMEM((rows, head_dim), jnp.bfloat16),
            pltpu.SemaphoreType.DMA((group + 1,)),
        ],
        compiler_params=params,
        name="bank",
    )(own, load, other, pick)
    return (relevance.transpose(1, 0, 2), bank[:, None, :])


def solution(mesh):
    return jax.shard_map(
        functools.partial(per_device, mesh.shape["seq"]),
        mesh=mesh,
        in_specs=(P("seq", "kvh", None), P("seq", "kvh", None), P("seq", "kvh", None), P(), P()),
        out_specs=(P("seq", "kvh", None), P("seq", "kvh", None)),
        check_vma=False,
    )
```

```python
import functools
import math

import jax
import jax.numpy as jnp
from jax import lax
from jax.experimental import pallas as pl
from jax.experimental.pallas import tpu as pltpu
from jax.sharding import PartitionSpec as P

BLK = 128
WIN = 512
PACK = 16
MIB = 1 << 20

VMEM = pl.BlockSpec(memory_space=pltpu.VMEM)
HBM = pl.BlockSpec(memory_space=pltpu.HBM)


def nt_dot(left, right):
    return lax.dot_general(
        left, right, (((1,), (1,)), ((), ())), preferred_element_type=jnp.float32
    )


def padded(rows, unit):
    return unit * pl.cdiv(rows, unit)


def key_order(parts):
    return sorted(range(1, parts), key=lambda k: (k % 2 == 0, k))


def lead_rows(parts):
    return padded(parts, PACK)


def term_rows(parts):
    return padded(3 * parts, PACK)


def unit(scale, query, keys):
    scores = nt_dot(keys, query)
    top = jnp.max(scores, axis=0, keepdims=True)
    grown = jnp.exp2((scores - top) * scale)
    return grown * (1.0 / jnp.sum(grown, axis=0, keepdims=True))


def column_sums(scale, query_ref, keys, inside):
    total = unit(scale, query_ref[0], keys)
    for head in range(1, query_ref.shape[0]):
        total += unit(scale, query_ref[head], keys)
    return total * inside


def representative(total, keys):
    column = jnp.sum(total, axis=1, keepdims=True)
    return jnp.sum(column * keys.astype(jnp.float32), axis=0, keepdims=True)


def first_kernel(
    parts, scale, start_hbm, slot_hbm, query_hbm, key_hbm,
    total_ref, mask_ref, pick_ref, query_ref, key_ref, start_ref, slot_ref, sems,
):
    tok = query_ref.shape[1]
    pairs = [(key_hbm, key_ref), (start_hbm, start_ref), (slot_hbm, slot_ref)]
    pairs.append((query_hbm, query_ref))
    copies = [pltpu.make_async_copy(*pair, sems.at[i]) for i, pair in enumerate(pairs)]
    for copy in copies:
        copy.start()
    me = lax.axis_index("seq")
    here, lane = me // 2, me % 2
    lead = lead_rows(parts)
    token = lax.broadcasted_iota(jnp.int32, (1, tok), 1)
    column = lax.broadcasted_iota(jnp.int32, (1, 2 * lead), 1)
    slots = jnp.full((1, 2 * lead), -1, jnp.int32)
    for copy in copies[:3]:
        copy.wait()
    for part in range(parts):
        for side in range(2):
            where = (me ^ side) * tok + token - start_ref[2 * part + lane]
            mask_ref[side, pl.ds(part, 1), :] = ((where >= 0) & (where < WIN)).astype(jnp.float32)
            slots = jnp.where(column == side * lead + part, slot_ref[2 * part + side], slots)
    row = lax.broadcasted_iota(jnp.int32, pick_ref.shape, 0)
    pick_ref[...] = (row == slots).astype(jnp.float32).astype(jnp.bfloat16)
    copies[3].wait()
    total_ref[...] = column_sums(scale, query_ref, key_ref[...], mask_ref[0, pl.ds(here, 1), :])


def own_kernel(part, scale, mask_ref, query_ref, key_ref, total_ref, pass_ref):
    pass_ref[...] = mask_ref[...]
    slot = (lax.axis_index("seq") // 2) ^ part
    inside = mask_ref[0, pl.ds(slot, 1), :]
    total_ref[...] = column_sums(scale, query_ref, key_ref[...], inside)


def mate_kernel(members, scale, mask_ref, query_ref, *refs):
    total_refs, key_refs, rep_ref = refs[: len(members)], refs[len(members) : -1], refs[-1]
    here = lax.axis_index("seq") // 2
    rep_ref[...] = jnp.zeros_like(rep_ref)
    for part, total_ref, key_ref in zip(members, total_refs, key_refs):
        slot = here ^ part
        keys = key_ref[...]
        total = column_sums(scale, query_ref, keys, mask_ref[1, pl.ds(slot, 1), :])
        rep_ref[pl.ds(slot, 1), :] = representative(total + total_ref[...], keys)


def last_kernel(
    parts, part, scale, mask_ref, prior_ref, own_ref, mate_ref, key_ref, sum_ref, rep_ref
):
    slot = (lax.axis_index("seq") // 2) ^ part
    keys = key_ref[...]
    rep_ref[...] = prior_ref[...]
    total = column_sums(scale, own_ref, keys, mask_ref[0, pl.ds(slot, 1), :])
    total += column_sums(scale, mate_ref, keys, mask_ref[1, pl.ds(slot, 1), :])
    rep_ref[pl.ds(slot, 1), :] = representative(total, keys)
    rest = rep_ref[pl.ds(0, parts), :]
    terms = []
    for _ in range(3):
        terms.append(rest.astype(jnp.bfloat16).astype(jnp.float32))
        rest = rest - terms[-1]
    spare = term_rows(parts) - 3 * parts
    if spare:
        terms.append(jnp.zeros((spare, rest.shape[1]), jnp.float32))
    sum_ref[...] = jnp.concatenate(terms, axis=0).astype(jnp.bfloat16)


def pair_kernel(own_ref, mate_ref, near_ref, far_ref, pair_ref):
    terms, rows = own_ref.shape[0], near_ref.shape[0]
    lane = lax.axis_index("seq") % 2
    for side, (sum_ref, cache_ref) in enumerate(((own_ref, near_ref), (mate_ref, far_ref))):
        start = pl.multiple_of((lane ^ side) * (terms + rows), PACK)
        pair_ref[pl.ds(start, terms), :] = sum_ref[...]
        pair_ref[pl.ds(pl.multiple_of(start + terms, PACK), rows), :] = cache_ref[...]


def bank_kernel(parts, share, scale, query_ref, pick_ref, *refs):
    pair_refs = refs[:parts]
    rel_ref, bank_ref, base_ref, rel_work, bank_work, sems = refs[parts:]
    group = query_ref.shape[0]
    rows = bank_ref.shape[0]
    lead, terms = lead_rows(parts), term_rows(parts)
    me = lax.axis_index("seq")
    fresh = []
    for side in range(2):
        first = side * (terms + rows)
        sums = []
        for part, ref in enumerate(pair_refs):
            wide = ref[pl.ds(first, terms), :].astype(jnp.float32)
            sums.append(wide[:parts] + (wide[parts : 2 * parts] + wide[2 * parts : 3 * parts]))
            start = pl.multiple_of((2 * ((me // 2) ^ part) + side) * rows, PACK)
            base_ref[pl.ds(start, rows), :] = ref[pl.ds(first + terms, rows), :]
        while len(sums) > 1:
            sums = [left + right for left, right in zip(sums[::2], sums[1::2])]
        fresh.append(sums[0] * share)
        if lead > parts:
            fresh.append(jnp.zeros((lead - parts, fresh[0].shape[1]), jnp.float32))
    fresh = jnp.concatenate(fresh, axis=0).astype(jnp.bfloat16)
    pick = pick_ref[...]
    placed = jnp.dot(pick, fresh, preferred_element_type=jnp.float32)
    taken = jnp.dot(pick, jnp.ones_like(fresh), preferred_element_type=jnp.float32)
    bank = jnp.where(taken > 0.5, placed, base_ref[...].astype(jnp.float32)).astype(jnp.bfloat16)
    base_ref[...] = bank
    bank_work[...] = base_ref[pl.ds(pl.multiple_of(me * rows, PACK), rows), :]
    copies = [pltpu.make_async_copy(bank_work, bank_ref, sems.at[group])]
    copies[0].start()
    for head in range(group):
        rel_work[head] = (nt_dot(query_ref[head], bank) * scale).astype(jnp.bfloat16)
        copies.append(pltpu.make_async_copy(rel_work.at[head], rel_ref.at[head], sems.at[head]))
        copies[-1].start()
    for copy in copies:
        copy.wait()


def per_device(count, queries, new_keys, cache_keys, window_start, owner_slot):
    tok, group, head_dim = queries.shape
    rows = cache_keys.shape[0]
    parts = count // 2
    lead = lead_rows(parts)
    assert tok == BLK and count == 1 << (count.bit_length() - 1) and count > 2
    score_scale = 1.0 / math.sqrt(head_dim)
    exp_scale = score_scale * math.log2(math.e)

    def swap(value, mask):
        return lax.ppermute(value, "seq", [(i, i ^ mask) for i in range(count)])

    def shape(rows_of, dtype):
        return jax.ShapeDtypeStruct((rows_of, head_dim), dtype)

    params = pltpu.CompilerParams(vmem_limit_bytes=(8 + parts) * MIB)
    asked = queries.transpose(1, 0, 2)
    keys = new_keys[:, 0, :]
    far = key_order(parts)
    mate = swap(asked, 1)
    pieces = {}
    for k in far:
        pieces[k] = swap(keys, 2 * k)

    cache = cache_keys[:, 0, :]
    far_cache = swap(cache, 1)
    square = jax.ShapeDtypeStruct((BLK, tok), jnp.float32)
    totals = {}
    totals[0], inside, pick, own, pieces[0] = pl.pallas_call(
        functools.partial(first_kernel, parts, exp_scale),
        out_shape=(
            square,
            jax.ShapeDtypeStruct((2, parts, tok), jnp.float32),
            jax.ShapeDtypeStruct((count * rows, 2 * lead), jnp.bfloat16),
            jax.ShapeDtypeStruct(asked.shape, jnp.bfloat16),
            jax.ShapeDtypeStruct(keys.shape, jnp.bfloat16),
        ),
        in_specs=[HBM] * 4,
        out_specs=(VMEM,) * 5,
        scratch_shapes=[
            pltpu.SMEM(window_start.shape, jnp.int32),
            pltpu.SMEM(owner_slot.shape, jnp.int32),
            pltpu.SemaphoreType.DMA((4,)),
        ],
        compiler_params=params,
        name="first",
    )(*[pltpu.with_memory_space_constraint(x, pltpu.HBM) for x in (window_start, owner_slot, asked, keys)])

    *middle, tail = far
    for k in middle:
        totals[k], inside = pl.pallas_call(
            functools.partial(own_kernel, k, exp_scale),
            out_shape=(square, inside),
            in_specs=[VMEM] * 3,
            out_specs=(VMEM, VMEM),
            compiler_params=params,
            name="own_step",
        )(inside, own, pieces[k])
    members = [0, *middle]
    partial = pl.pallas_call(
        functools.partial(mate_kernel, members, exp_scale),
        out_shape=shape(padded(parts, 8), jnp.float32),
        in_specs=[VMEM] * (2 + 2 * len(members)),
        out_specs=VMEM,
        compiler_params=params,
        name="mate_step",
    )(inside, mate, *[totals[k] for k in members], *[pieces[k] for k in members])
    partial = pl.pallas_call(
        functools.partial(last_kernel, parts, tail, exp_scale),
        out_shape=shape(term_rows(parts), jnp.bfloat16),
        in_specs=[VMEM] * 5,
        out_specs=VMEM,
        scratch_shapes=[pltpu.VMEM((padded(parts, 8), head_dim), jnp.float32)],
        compiler_params=params,
        name="last",
    )(inside, partial, own, mate, pieces[tail])

    other = swap(partial, 1)
    pair = pl.pallas_call(
        pair_kernel,
        out_shape=shape(2 * (partial.shape[0] + rows), jnp.bfloat16),
        in_specs=[VMEM] * 4,
        out_specs=VMEM,
        compiler_params=params,
        name="pair",
    )(partial, other, cache, far_cache)
    pairs = [pair]
    for k in range(1, parts):
        pairs.append(swap(pair, 2 * k))

    relevance, bank = pl.pallas_call(
        functools.partial(bank_kernel, parts, 1.0 / (group * WIN), score_scale),
        out_shape=(
            jax.ShapeDtypeStruct((group, tok, count * rows), jnp.bfloat16),
            jax.ShapeDtypeStruct((rows, head_dim), jnp.bfloat16),
        ),
        in_specs=[VMEM] * (2 + parts),
        out_specs=(HBM, HBM),
        scratch_shapes=[
            pltpu.VMEM((count * rows, head_dim), jnp.bfloat16),
            pltpu.VMEM((group, tok, count * rows), jnp.bfloat16),
            pltpu.VMEM((rows, head_dim), jnp.bfloat16),
            pltpu.SemaphoreType.DMA((group + 1,)),
        ],
        compiler_params=params,
        name="bank",
    )(own, pick, *pairs)
    return (relevance.transpose(1, 0, 2), bank[:, None, :])


def solution(mesh):
    count = mesh.shape["seq"]

    def body(*args):
        return per_device(count, *args)

    return jax.shard_map(
        body,
        mesh=mesh,
        in_specs=(P("seq", "kvh", None), P("seq", "kvh", None), P("seq", "kvh", None), P(), P()),
        out_specs=(P("seq", "kvh", None), P("seq", "kvh", None)),
        check_vma=False,
    )
```

```python
import functools
import math

import jax
import jax.numpy as jnp
from jax import lax
from jax.experimental import pallas as pl
from jax.experimental.pallas import tpu as pltpu
from jax.sharding import PartitionSpec as P

BLK = 128
WIN = 512
PACK = 16
MIB = 1 << 20

VMEM = pl.BlockSpec(memory_space=pltpu.VMEM)
HBM = pl.BlockSpec(memory_space=pltpu.HBM)


def nt_dot(left, right):
    return lax.dot_general(
        left, right, (((1,), (1,)), ((), ())), preferred_element_type=jnp.float32
    )


def padded(rows, unit):
    return unit * pl.cdiv(rows, unit)


def key_order(parts):
    return sorted(range(1, parts), key=lambda k: (k % 2 == 0, k))


def lead_rows(parts):
    return padded(parts, PACK)


def term_rows(parts):
    return padded(3 * parts, PACK)


def unit(scale, query, keys):
    scores = nt_dot(keys, query)
    top = jnp.max(scores, axis=0, keepdims=True)
    grown = jnp.exp2((scores - top) * scale)
    return grown * (1.0 / jnp.sum(grown, axis=0, keepdims=True))


def column_sums(scale, query_ref, keys, inside):
    total = unit(scale, query_ref[0], keys)
    for head in range(1, query_ref.shape[0]):
        total += unit(scale, query_ref[head], keys)
    return total * inside


def representative(total, keys):
    column = jnp.sum(total, axis=1, keepdims=True)
    return jnp.sum(column * keys.astype(jnp.float32), axis=0, keepdims=True)


def first_kernel(
    parts, scale, start_hbm, slot_hbm, query_hbm, key_hbm,
    total_ref, mask_ref, pick_ref, query_ref, key_ref, start_ref, slot_ref, sems,
):
    tok = query_ref.shape[1]
    pairs = [(key_hbm, key_ref), (start_hbm, start_ref), (slot_hbm, slot_ref)]
    pairs += [(query_hbm.at[head], query_ref.at[head]) for head in range(query_ref.shape[0])]
    copies = [pltpu.make_async_copy(*pair, sems.at[i]) for i, pair in enumerate(pairs)]
    for copy in copies:
        copy.start()
    me = lax.axis_index("seq")
    here, lane = me // 2, me % 2
    lead = lead_rows(parts)
    token = lax.broadcasted_iota(jnp.int32, (1, tok), 1)
    column = lax.broadcasted_iota(jnp.int32, (1, 2 * lead), 1)
    slots = jnp.full((1, 2 * lead), -1, jnp.int32)
    for copy in copies[:3]:
        copy.wait()
    for part in range(parts):
        for side in range(2):
            where = (me ^ side) * tok + token - start_ref[2 * part + lane]
            mask_ref[side, pl.ds(part, 1), :] = ((where >= 0) & (where < WIN)).astype(jnp.float32)
            slots = jnp.where(column == side * lead + part, slot_ref[2 * part + side], slots)
    row = lax.broadcasted_iota(jnp.int32, pick_ref.shape, 0)
    pick_ref[...] = (row == slots).astype(jnp.float32).astype(jnp.bfloat16)
    for copy in copies[3:]:
        copy.wait()
    total_ref[...] = column_sums(scale, query_ref, key_ref[...], mask_ref[0, pl.ds(here, 1), :])


def own_kernel(part, scale, mask_ref, query_ref, key_ref, total_ref, pass_ref):
    pass_ref[...] = mask_ref[...]
    slot = (lax.axis_index("seq") // 2) ^ part
    inside = mask_ref[0, pl.ds(slot, 1), :]
    total_ref[...] = column_sums(scale, query_ref, key_ref[...], inside)


def mate_kernel(members, scale, mask_ref, query_ref, *refs):
    total_refs, key_refs, rep_ref = refs[: len(members)], refs[len(members) : -1], refs[-1]
    here = lax.axis_index("seq") // 2
    rep_ref[...] = jnp.zeros_like(rep_ref)
    for part, total_ref, key_ref in zip(members, total_refs, key_refs):
        slot = here ^ part
        keys = key_ref[...]
        total = column_sums(scale, query_ref, keys, mask_ref[1, pl.ds(slot, 1), :])
        rep_ref[pl.ds(slot, 1), :] = representative(total + total_ref[...], keys)


def last_kernel(
    parts, part, scale, mask_ref, prior_ref, own_ref, mate_ref, key_ref, sum_ref, rep_ref
):
    slot = (lax.axis_index("seq") // 2) ^ part
    keys = key_ref[...]
    rep_ref[...] = prior_ref[...]
    total = column_sums(scale, own_ref, keys, mask_ref[0, pl.ds(slot, 1), :])
    total += column_sums(scale, mate_ref, keys, mask_ref[1, pl.ds(slot, 1), :])
    rep_ref[pl.ds(slot, 1), :] = representative(total, keys)
    rest = rep_ref[pl.ds(0, parts), :]
    terms = []
    for _ in range(3):
        terms.append(rest.astype(jnp.bfloat16).astype(jnp.float32))
        rest = rest - terms[-1]
    spare = term_rows(parts) - 3 * parts
    if spare:
        terms.append(jnp.zeros((spare, rest.shape[1]), jnp.float32))
    sum_ref[...] = jnp.concatenate(terms, axis=0).astype(jnp.bfloat16)


def pair_kernel(own_ref, mate_ref, near_ref, far_ref, pair_ref):
    terms, rows = own_ref.shape[0], near_ref.shape[0]
    lane = lax.axis_index("seq") % 2
    for side, (sum_ref, cache_ref) in enumerate(((own_ref, near_ref), (mate_ref, far_ref))):
        start = pl.multiple_of((lane ^ side) * (terms + rows), PACK)
        pair_ref[pl.ds(start, terms), :] = sum_ref[...]
        pair_ref[pl.ds(pl.multiple_of(start + terms, PACK), rows), :] = cache_ref[...]


def bank_kernel(parts, share, scale, query_ref, pick_ref, *refs):
    pair_refs = refs[:parts]
    rel_ref, bank_ref, base_ref, rel_work, bank_work, sems = refs[parts:]
    group = query_ref.shape[0]
    rows = bank_ref.shape[0]
    lead, terms = lead_rows(parts), term_rows(parts)
    me = lax.axis_index("seq")
    fresh = []
    for side in range(2):
        first = side * (terms + rows)
        sums = []
        for part, ref in enumerate(pair_refs):
            wide = ref[pl.ds(first, terms), :].astype(jnp.float32)
            sums.append(wide[:parts] + (wide[parts : 2 * parts] + wide[2 * parts : 3 * parts]))
            start = pl.multiple_of((2 * ((me // 2) ^ part) + side) * rows, PACK)
            base_ref[pl.ds(start, rows), :] = ref[pl.ds(first + terms, rows), :]
        while len(sums) > 1:
            sums = [left + right for left, right in zip(sums[::2], sums[1::2])]
        fresh.append(sums[0] * share)
        if lead > parts:
            fresh.append(jnp.zeros((lead - parts, fresh[0].shape[1]), jnp.float32))
    fresh = jnp.concatenate(fresh, axis=0).astype(jnp.bfloat16)
    pick = pick_ref[...]
    placed = jnp.dot(pick, fresh, preferred_element_type=jnp.float32)
    taken = jnp.dot(pick, jnp.ones_like(fresh), preferred_element_type=jnp.float32)
    bank = jnp.where(taken > 0.5, placed, base_ref[...].astype(jnp.float32)).astype(jnp.bfloat16)
    base_ref[...] = bank
    bank_work[...] = base_ref[pl.ds(pl.multiple_of(me * rows, PACK), rows), :]
    copies = [pltpu.make_async_copy(bank_work, bank_ref, sems.at[group])]
    copies[0].start()
    for head in range(group):
        rel_work[head] = (nt_dot(query_ref[head], bank) * scale).astype(jnp.bfloat16)
        copies.append(pltpu.make_async_copy(rel_work.at[head], rel_ref.at[head], sems.at[head]))
        copies[-1].start()
    for copy in copies:
        copy.wait()


def per_device(count, queries, new_keys, cache_keys, window_start, owner_slot):
    tok, group, head_dim = queries.shape
    rows = cache_keys.shape[0]
    parts = count // 2
    lead = lead_rows(parts)
    assert tok == BLK and count == 1 << (count.bit_length() - 1) and count > 2
    score_scale = 1.0 / math.sqrt(head_dim)
    exp_scale = score_scale * math.log2(math.e)

    def swap(value, mask):
        return lax.ppermute(value, "seq", [(i, i ^ mask) for i in range(count)])

    def shape(rows_of, dtype):
        return jax.ShapeDtypeStruct((rows_of, head_dim), dtype)

    params = pltpu.CompilerParams(vmem_limit_bytes=(8 + parts) * MIB)
    asked = queries.transpose(1, 0, 2)
    keys = new_keys[:, 0, :]
    far = key_order(parts)
    mate = swap(asked, 1)
    pieces = {}
    for k in far:
        pieces[k] = swap(keys, 2 * k)

    cache = cache_keys[:, 0, :]
    far_cache = swap(cache, 1)
    square = jax.ShapeDtypeStruct((BLK, tok), jnp.float32)
    totals = {}
    totals[0], inside, pick, own, pieces[0] = pl.pallas_call(
        functools.partial(first_kernel, parts, exp_scale),
        out_shape=(
            square,
            jax.ShapeDtypeStruct((2, parts, tok), jnp.float32),
            jax.ShapeDtypeStruct((count * rows, 2 * lead), jnp.bfloat16),
            jax.ShapeDtypeStruct(asked.shape, jnp.bfloat16),
            jax.ShapeDtypeStruct(keys.shape, jnp.bfloat16),
        ),
        in_specs=[HBM] * 4,
        out_specs=(VMEM,) * 5,
        scratch_shapes=[
            pltpu.SMEM(window_start.shape, jnp.int32),
            pltpu.SMEM(owner_slot.shape, jnp.int32),
            pltpu.SemaphoreType.DMA((3 + group,)),
        ],
        compiler_params=params,
        name="first",
    )(*[pltpu.with_memory_space_constraint(x, pltpu.HBM) for x in (window_start, owner_slot, asked, keys)])

    *middle, tail = far
    for k in middle:
        totals[k], inside = pl.pallas_call(
            functools.partial(own_kernel, k, exp_scale),
            out_shape=(square, inside),
            in_specs=[VMEM] * 3,
            out_specs=(VMEM, VMEM),
            compiler_params=params,
            name="own_step",
        )(inside, own, pieces[k])
    members = [0, *middle]
    partial = pl.pallas_call(
        functools.partial(mate_kernel, members, exp_scale),
        out_shape=shape(padded(parts, 8), jnp.float32),
        in_specs=[VMEM] * (2 + 2 * len(members)),
        out_specs=VMEM,
        compiler_params=params,
        name="mate_step",
    )(inside, mate, *[totals[k] for k in members], *[pieces[k] for k in members])
    partial = pl.pallas_call(
        functools.partial(last_kernel, parts, tail, exp_scale),
        out_shape=shape(term_rows(parts), jnp.bfloat16),
        in_specs=[VMEM] * 5,
        out_specs=VMEM,
        scratch_shapes=[pltpu.VMEM((padded(parts, 8), head_dim), jnp.float32)],
        compiler_params=params,
        name="last",
    )(inside, partial, own, mate, pieces[tail])

    other = swap(partial, 1)
    pair = pl.pallas_call(
        pair_kernel,
        out_shape=shape(2 * (partial.shape[0] + rows), jnp.bfloat16),
        in_specs=[VMEM] * 4,
        out_specs=VMEM,
        compiler_params=params,
        name="pair",
    )(partial, other, cache, far_cache)
    pairs = [pair]
    for k in range(1, parts):
        pairs.append(swap(pair, 2 * k))

    relevance, bank = pl.pallas_call(
        functools.partial(bank_kernel, parts, 1.0 / (group * WIN), score_scale),
        out_shape=(
            jax.ShapeDtypeStruct((group, tok, count * rows), jnp.bfloat16),
            jax.ShapeDtypeStruct((rows, head_dim), jnp.bfloat16),
        ),
        in_specs=[VMEM] * (2 + parts),
        out_specs=(HBM, HBM),
        scratch_shapes=[
            pltpu.VMEM((count * rows, head_dim), jnp.bfloat16),
            pltpu.VMEM((group, tok, count * rows), jnp.bfloat16),
            pltpu.VMEM((rows, head_dim), jnp.bfloat16),
            pltpu.SemaphoreType.DMA((group + 1,)),
        ],
        compiler_params=params,
        name="bank",
    )(own, pick, *pairs)
    return (relevance.transpose(1, 0, 2), bank[:, None, :])


def solution(mesh):
    count = mesh.shape["seq"]

    def body(*args):
        return per_device(count, *args)

    return jax.shard_map(
        body,
        mesh=mesh,
        in_specs=(P("seq", "kvh", None), P("seq", "kvh", None), P("seq", "kvh", None), P(), P()),
        out_specs=(P("seq", "kvh", None), P("seq", "kvh", None)),
        check_vma=False,
    )
```

```python
import functools
import math

import jax
import jax.numpy as jnp
from jax import lax
from jax.experimental import pallas as pl
from jax.experimental.pallas import tpu as pltpu
from jax.sharding import PartitionSpec as P

BLK = 128
WIN = 512
PACK = 16
MIB = 1 << 20

VMEM = pl.BlockSpec(memory_space=pltpu.VMEM)
HBM = pl.BlockSpec(memory_space=pltpu.HBM)


def nt_dot(left, right):
    return lax.dot_general(
        left, right, (((1,), (1,)), ((), ())), preferred_element_type=jnp.float32
    )


def padded(rows, unit):
    return unit * pl.cdiv(rows, unit)


def key_order(parts):
    return sorted(range(1, parts), key=lambda k: (k % 2 == 0, k))


def sum_order(parts):
    return sorted(range(1, parts), key=lambda k: (k % 2 == 0, -k))


def lead_rows(parts):
    return padded(parts, PACK)


def term_rows(parts):
    return padded(3 * parts, PACK)


def unit(scale, query, keys):
    scores = nt_dot(keys, query)
    top = jnp.max(scores, axis=0, keepdims=True)
    grown = jnp.exp2((scores - top) * scale)
    return grown * (1.0 / jnp.sum(grown, axis=0, keepdims=True))


def column_sums(scale, query_ref, keys, inside):
    total = unit(scale, query_ref[0], keys)
    for head in range(1, query_ref.shape[0]):
        total += unit(scale, query_ref[head], keys)
    return total * inside


def representative(total, keys):
    column = jnp.sum(total, axis=1, keepdims=True)
    return jnp.sum(column * keys.astype(jnp.float32), axis=0, keepdims=True)


def first_kernel(
    parts, scale, start_hbm, slot_hbm, query_hbm, key_hbm,
    total_ref, mask_ref, pick_ref, query_ref, key_ref, start_ref, slot_ref, sems,
):
    tok = query_ref.shape[1]
    pairs = [(key_hbm, key_ref), (start_hbm, start_ref), (slot_hbm, slot_ref)]
    pairs += [(query_hbm.at[head], query_ref.at[head]) for head in range(query_ref.shape[0])]
    copies = [pltpu.make_async_copy(*pair, sems.at[i]) for i, pair in enumerate(pairs)]
    for copy in copies:
        copy.start()
    me = lax.axis_index("seq")
    here, lane = me // 2, me % 2
    lead = lead_rows(parts)
    token = lax.broadcasted_iota(jnp.int32, (1, tok), 1)
    column = lax.broadcasted_iota(jnp.int32, (1, 2 * lead), 1)
    slots = jnp.full((1, 2 * lead), -1, jnp.int32)
    for copy in copies[:3]:
        copy.wait()
    for part in range(parts):
        for side in range(2):
            where = (me ^ side) * tok + token - start_ref[2 * part + lane]
            mask_ref[side, pl.ds(part, 1), :] = ((where >= 0) & (where < WIN)).astype(jnp.float32)
            slots = jnp.where(column == side * lead + part, slot_ref[2 * part + side], slots)
    row = lax.broadcasted_iota(jnp.int32, pick_ref.shape, 0)
    pick_ref[...] = (row == slots).astype(jnp.float32).astype(jnp.bfloat16)
    for copy in copies[3:]:
        copy.wait()
    total_ref[...] = column_sums(scale, query_ref, key_ref[...], mask_ref[0, pl.ds(here, 1), :])


def own_kernel(part, scale, mask_ref, query_ref, key_ref, total_ref, pass_ref):
    pass_ref[...] = mask_ref[...]
    slot = (lax.axis_index("seq") // 2) ^ part
    inside = mask_ref[0, pl.ds(slot, 1), :]
    total_ref[...] = column_sums(scale, query_ref, key_ref[...], inside)


def mate_kernel(members, scale, mask_ref, query_ref, *refs):
    total_refs, key_refs, rep_ref = refs[: len(members)], refs[len(members) : -1], refs[-1]
    here = lax.axis_index("seq") // 2
    rep_ref[...] = jnp.zeros_like(rep_ref)
    for part, total_ref, key_ref in zip(members, total_refs, key_refs):
        slot = here ^ part
        keys = key_ref[...]
        total = column_sums(scale, query_ref, keys, mask_ref[1, pl.ds(slot, 1), :])
        rep_ref[pl.ds(slot, 1), :] = representative(total + total_ref[...], keys)


def last_kernel(
    parts, part, scale, mask_ref, prior_ref, own_ref, mate_ref, key_ref, sum_ref, rep_ref
):
    slot = (lax.axis_index("seq") // 2) ^ part
    keys = key_ref[...]
    rep_ref[...] = prior_ref[...]
    total = column_sums(scale, own_ref, keys, mask_ref[0, pl.ds(slot, 1), :])
    total += column_sums(scale, mate_ref, keys, mask_ref[1, pl.ds(slot, 1), :])
    rep_ref[pl.ds(slot, 1), :] = representative(total, keys)
    rest = rep_ref[pl.ds(0, parts), :]
    terms = []
    for _ in range(3):
        terms.append(rest.astype(jnp.bfloat16).astype(jnp.float32))
        rest = rest - terms[-1]
    spare = term_rows(parts) - 3 * parts
    if spare:
        terms.append(jnp.zeros((spare, rest.shape[1]), jnp.float32))
    sum_ref[...] = jnp.concatenate(terms, axis=0).astype(jnp.bfloat16)


def pair_kernel(own_ref, mate_ref, near_ref, far_ref, pair_ref):
    terms, rows = own_ref.shape[0], near_ref.shape[0]
    lane = lax.axis_index("seq") % 2
    for side, (sum_ref, cache_ref) in enumerate(((own_ref, near_ref), (mate_ref, far_ref))):
        start = pl.multiple_of((lane ^ side) * (terms + rows), PACK)
        pair_ref[pl.ds(start, terms), :] = sum_ref[...]
        pair_ref[pl.ds(pl.multiple_of(start + terms, PACK), rows), :] = cache_ref[...]


def pair_sums(parts, ref):
    terms = term_rows(parts)
    half = ref.shape[0] // 2
    sums = []
    for side in range(2):
        wide = ref[pl.ds(side * half, terms), :].astype(jnp.float32)
        sums.append(wide[:parts] + (wide[parts : 2 * parts] + wide[2 * parts : 3 * parts]))
    return sums


def pair_rows(parts, ref):
    terms, half = term_rows(parts), ref.shape[0] // 2
    return jnp.concatenate(
        [ref[pl.ds(terms, half - terms), :], ref[pl.ds(half + terms, half - terms), :]], axis=0
    )


def prep_kernel(parts, members, pick_ref, *refs):
    pair_refs = refs[: len(members)]
    base_ref, keep_ref, sum_ref = refs[len(members) :]
    here = lax.axis_index("seq") // 2
    pick = pick_ref[...]
    ones = jnp.ones((pick.shape[1], base_ref.shape[1]), jnp.bfloat16)
    taken = jnp.dot(pick, ones, preferred_element_type=jnp.float32)
    keep_ref[...] = (1.0 - taken).astype(jnp.bfloat16)
    base_ref[...] = jnp.zeros_like(base_ref)
    for index, (part, ref) in enumerate(zip(members, pair_refs)):
        rows = pair_rows(parts, ref)
        span = pl.ds(pl.multiple_of((here ^ part) * rows.shape[0], PACK), rows.shape[0])
        base_ref[span, :] = rows * keep_ref[span, :]
        for side, value in enumerate(pair_sums(parts, ref)):
            sum_ref[index, side, pl.ds(0, parts), :] = value


def bank_kernel(
    parts, members, late, share, scale, query_ref, pick_ref, ready_ref, keep_ref, sum_ref, pair_ref,
    rel_ref, bank_ref, base_ref, rel_work, bank_work, sems,
):
    group = query_ref.shape[0]
    rows = bank_ref.shape[0]
    lead = lead_rows(parts)
    me = lax.axis_index("seq")
    base_ref[...] = ready_ref[...]
    span = pl.ds(pl.multiple_of(((me // 2) ^ late) * 2 * rows, PACK), 2 * rows)
    base_ref[span, :] = pair_rows(parts, pair_ref) * keep_ref[span, :]
    fresh = []
    for side, last in enumerate(pair_sums(parts, pair_ref)):
        sums = {late: last}
        for index, part in enumerate(members):
            sums[part] = sum_ref[index, side, pl.ds(0, parts), :]
        sums = [sums[part] for part in range(parts)]
        while len(sums) > 1:
            sums = [left + right for left, right in zip(sums[::2], sums[1::2])]
        fresh.append(sums[0] * share)
        if lead > parts:
            fresh.append(jnp.zeros((lead - parts, fresh[0].shape[1]), jnp.float32))
    fresh = jnp.concatenate(fresh, axis=0).astype(jnp.bfloat16)
    placed = jnp.dot(pick_ref[...], fresh, preferred_element_type=jnp.float32)
    bank = base_ref[...] + placed.astype(jnp.bfloat16)
    base_ref[...] = bank
    bank_work[...] = base_ref[pl.ds(pl.multiple_of(me * rows, PACK), rows), :]
    copies = [pltpu.make_async_copy(bank_work, bank_ref, sems.at[group])]
    copies[0].start()
    for head in range(group):
        rel_work[head] = (nt_dot(query_ref[head], bank) * scale).astype(jnp.bfloat16)
        copies.append(pltpu.make_async_copy(rel_work.at[head], rel_ref.at[head], sems.at[head]))
        copies[-1].start()
    for copy in copies:
        copy.wait()


def per_device(count, queries, new_keys, cache_keys, window_start, owner_slot):
    tok, group, head_dim = queries.shape
    rows = cache_keys.shape[0]
    parts = count // 2
    lead = lead_rows(parts)
    assert tok == BLK and count == 1 << (count.bit_length() - 1) and count > 2
    score_scale = 1.0 / math.sqrt(head_dim)
    exp_scale = score_scale * math.log2(math.e)

    def swap(value, mask):
        return lax.ppermute(value, "seq", [(i, i ^ mask) for i in range(count)])

    def shape(rows_of, dtype):
        return jax.ShapeDtypeStruct((rows_of, head_dim), dtype)

    params = pltpu.CompilerParams(vmem_limit_bytes=(8 + parts) * MIB)
    asked = queries.transpose(1, 0, 2)
    keys = new_keys[:, 0, :]
    far = key_order(parts)
    mate = swap(asked, 1)
    pieces = {}
    for k in far:
        pieces[k] = swap(keys, 2 * k)

    cache = cache_keys[:, 0, :]
    far_cache = swap(cache, 1)
    square = jax.ShapeDtypeStruct((BLK, tok), jnp.float32)
    totals = {}
    totals[0], inside, pick, own, pieces[0] = pl.pallas_call(
        functools.partial(first_kernel, parts, exp_scale),
        out_shape=(
            square,
            jax.ShapeDtypeStruct((2, parts, tok), jnp.float32),
            jax.ShapeDtypeStruct((count * rows, 2 * lead), jnp.bfloat16),
            jax.ShapeDtypeStruct(asked.shape, jnp.bfloat16),
            jax.ShapeDtypeStruct(keys.shape, jnp.bfloat16),
        ),
        in_specs=[HBM] * 4,
        out_specs=(VMEM,) * 5,
        scratch_shapes=[
            pltpu.SMEM(window_start.shape, jnp.int32),
            pltpu.SMEM(owner_slot.shape, jnp.int32),
            pltpu.SemaphoreType.DMA((3 + group,)),
        ],
        compiler_params=params,
        name="first",
    )(*[pltpu.with_memory_space_constraint(x, pltpu.HBM) for x in (window_start, owner_slot, asked, keys)])

    *middle, tail = far
    for k in middle:
        totals[k], inside = pl.pallas_call(
            functools.partial(own_kernel, k, exp_scale),
            out_shape=(square, inside),
            in_specs=[VMEM] * 3,
            out_specs=(VMEM, VMEM),
            compiler_params=params,
            name="own_step",
        )(inside, own, pieces[k])
    members = [0, *middle]
    partial = pl.pallas_call(
        functools.partial(mate_kernel, members, exp_scale),
        out_shape=shape(padded(parts, 8), jnp.float32),
        in_specs=[VMEM] * (2 + 2 * len(members)),
        out_specs=VMEM,
        compiler_params=params,
        name="mate_step",
    )(inside, mate, *[totals[k] for k in members], *[pieces[k] for k in members])
    partial = pl.pallas_call(
        functools.partial(last_kernel, parts, tail, exp_scale),
        out_shape=shape(term_rows(parts), jnp.bfloat16),
        in_specs=[VMEM] * 5,
        out_specs=VMEM,
        scratch_shapes=[pltpu.VMEM((padded(parts, 8), head_dim), jnp.float32)],
        compiler_params=params,
        name="last",
    )(inside, partial, own, mate, pieces[tail])

    other = swap(partial, 1)
    pair = pl.pallas_call(
        pair_kernel,
        out_shape=shape(2 * (partial.shape[0] + rows), jnp.bfloat16),
        in_specs=[VMEM] * 4,
        out_specs=VMEM,
        compiler_params=params,
        name="pair",
    )(partial, other, cache, far_cache)
    pairs = [pair]
    for k in range(1, parts):
        pairs.append(swap(pair, 2 * k))

    *members, late = [0, *sum_order(parts)]
    ready, keep, sums = pl.pallas_call(
        functools.partial(prep_kernel, parts, members),
        out_shape=(
            shape(count * rows, jnp.bfloat16),
            shape(count * rows, jnp.bfloat16),
            jax.ShapeDtypeStruct((len(members), 2, padded(parts, 8), head_dim), jnp.float32),
        ),
        in_specs=[VMEM] * (1 + len(members)),
        out_specs=(VMEM,) * 3,
        compiler_params=params,
        name="prep",
    )(pick, *[pairs[part] for part in members])

    relevance, bank = pl.pallas_call(
        functools.partial(bank_kernel, parts, members, late, 1.0 / (group * WIN), score_scale),
        out_shape=(
            jax.ShapeDtypeStruct((group, tok, count * rows), jnp.bfloat16),
            jax.ShapeDtypeStruct((rows, head_dim), jnp.bfloat16),
        ),
        in_specs=[VMEM] * 6,
        out_specs=(HBM, HBM),
        scratch_shapes=[
            pltpu.VMEM((count * rows, head_dim), jnp.bfloat16),
            pltpu.VMEM((group, tok, count * rows), jnp.bfloat16),
            pltpu.VMEM((rows, head_dim), jnp.bfloat16),
            pltpu.SemaphoreType.DMA((group + 1,)),
        ],
        compiler_params=params,
        name="bank",
    )(own, pick, ready, keep, sums, pairs[late])
    return (relevance.transpose(1, 0, 2), bank[:, None, :])


def solution(mesh):
    count = mesh.shape["seq"]

    def body(*args):
        return per_device(count, *args)

    return jax.shard_map(
        body,
        mesh=mesh,
        in_specs=(P("seq", "kvh", None), P("seq", "kvh", None), P("seq", "kvh", None), P(), P()),
        out_specs=(P("seq", "kvh", None), P("seq", "kvh", None)),
        check_vma=False,
    )
```

```python
import functools
import math

import jax
import jax.numpy as jnp
from jax import lax
from jax.experimental import pallas as pl
from jax.experimental.pallas import tpu as pltpu
from jax.sharding import PartitionSpec as P

BLK = 128
WIN = 512
PACK = 16
MIB = 1 << 20

VMEM = pl.BlockSpec(memory_space=pltpu.VMEM)
HBM = pl.BlockSpec(memory_space=pltpu.HBM)


def nt_dot(left, right):
    return lax.dot_general(
        left, right, (((1,), (1,)), ((), ())), preferred_element_type=jnp.float32
    )


def padded(rows, unit):
    return unit * pl.cdiv(rows, unit)


def key_order(parts):
    return sorted(range(1, parts), key=lambda k: (k % 2 == 0, k))


def sum_order(parts):
    return sorted(range(1, parts), key=lambda k: (k % 2 == 0, -k))


def lead_rows(parts):
    return padded(parts, PACK)


def term_rows(parts):
    return padded(3 * parts, PACK)


def unit(scale, query, keys):
    scores = nt_dot(keys, query)
    top = jnp.max(scores, axis=0, keepdims=True)
    grown = jnp.exp2((scores - top) * scale)
    return grown * (1.0 / jnp.sum(grown, axis=0, keepdims=True))


def column_sums(scale, query_ref, keys, inside):
    total = unit(scale, query_ref[0], keys)
    for head in range(1, query_ref.shape[0]):
        total += unit(scale, query_ref[head], keys)
    return total * inside


def representative(total, keys):
    column = jnp.sum(total, axis=1, keepdims=True)
    return jnp.sum(column * keys.astype(jnp.float32), axis=0, keepdims=True)


def first_kernel(
    parts, scale, start_hbm, slot_hbm, query_hbm, key_hbm,
    total_ref, mask_ref, pick_ref, query_ref, key_ref, start_ref, slot_ref, sems,
):
    tok = query_ref.shape[1]
    pairs = [(key_hbm, key_ref), (start_hbm, start_ref), (slot_hbm, slot_ref)]
    pairs += [(query_hbm.at[head], query_ref.at[head]) for head in range(query_ref.shape[0])]
    copies = [pltpu.make_async_copy(*pair, sems.at[i]) for i, pair in enumerate(pairs)]
    for copy in copies:
        copy.start()
    me = lax.axis_index("seq")
    here, lane = me // 2, me % 2
    lead = lead_rows(parts)
    token = lax.broadcasted_iota(jnp.int32, (1, tok), 1)
    column = lax.broadcasted_iota(jnp.int32, (1, 2 * lead), 1)
    slots = jnp.full((1, 2 * lead), -1, jnp.int32)
    for copy in copies[:3]:
        copy.wait()
    for part in range(parts):
        for side in range(2):
            where = (me ^ side) * tok + token - start_ref[2 * part + lane]
            mask_ref[side, pl.ds(part, 1), :] = ((where >= 0) & (where < WIN)).astype(jnp.float32)
            slots = jnp.where(column == side * lead + part, slot_ref[2 * part + side], slots)
    row = lax.broadcasted_iota(jnp.int32, pick_ref.shape, 0)
    pick_ref[...] = (row == slots).astype(jnp.float32).astype(jnp.bfloat16)
    for copy in copies[3:]:
        copy.wait()
    total_ref[...] = column_sums(scale, query_ref, key_ref[...], mask_ref[0, pl.ds(here, 1), :])


def own_kernel(part, scale, mask_ref, query_ref, key_ref, total_ref):
    slot = (lax.axis_index("seq") // 2) ^ part
    inside = mask_ref[0, pl.ds(slot, 1), :]
    total_ref[...] = column_sums(scale, query_ref, key_ref[...], inside)


def mate_kernel(members, scale, mask_ref, query_ref, *refs):
    total_refs, key_refs, rep_ref = refs[: len(members)], refs[len(members) : -1], refs[-1]
    here = lax.axis_index("seq") // 2
    rep_ref[...] = jnp.zeros_like(rep_ref)
    for part, total_ref, key_ref in zip(members, total_refs, key_refs):
        slot = here ^ part
        keys = key_ref[...]
        total = column_sums(scale, query_ref, keys, mask_ref[1, pl.ds(slot, 1), :])
        rep_ref[pl.ds(slot, 1), :] = representative(total + total_ref[...], keys)


def last_kernel(
    parts, part, scale, mask_ref, prior_ref, own_ref, mate_ref, key_ref, sum_ref, rep_ref
):
    slot = (lax.axis_index("seq") // 2) ^ part
    keys = key_ref[...]
    rep_ref[...] = prior_ref[...]
    total = column_sums(scale, own_ref, keys, mask_ref[0, pl.ds(slot, 1), :])
    total += column_sums(scale, mate_ref, keys, mask_ref[1, pl.ds(slot, 1), :])
    rep_ref[pl.ds(slot, 1), :] = representative(total, keys)
    rest = rep_ref[pl.ds(0, parts), :]
    terms = []
    for _ in range(3):
        terms.append(rest.astype(jnp.bfloat16).astype(jnp.float32))
        rest = rest - terms[-1]
    spare = term_rows(parts) - 3 * parts
    if spare:
        terms.append(jnp.zeros((spare, rest.shape[1]), jnp.float32))
    sum_ref[...] = jnp.concatenate(terms, axis=0).astype(jnp.bfloat16)


def pair_kernel(own_ref, mate_ref, near_ref, far_ref, pair_ref):
    terms, rows = own_ref.shape[0], near_ref.shape[0]
    lane = lax.axis_index("seq") % 2
    for side, (sum_ref, cache_ref) in enumerate(((own_ref, near_ref), (mate_ref, far_ref))):
        start = pl.multiple_of((lane ^ side) * (terms + rows), PACK)
        pair_ref[pl.ds(start, terms), :] = sum_ref[...]
        pair_ref[pl.ds(pl.multiple_of(start + terms, PACK), rows), :] = cache_ref[...]


def pair_sums(parts, ref):
    terms = term_rows(parts)
    half = ref.shape[0] // 2
    sums = []
    for side in range(2):
        wide = ref[pl.ds(side * half, terms), :].astype(jnp.float32)
        sums.append(wide[:parts] + (wide[parts : 2 * parts] + wide[2 * parts : 3 * parts]))
    return sums


def pair_rows(parts, ref):
    terms, half = term_rows(parts), ref.shape[0] // 2
    return jnp.concatenate(
        [ref[pl.ds(terms, half - terms), :], ref[pl.ds(half + terms, half - terms), :]], axis=0
    )


def prep_kernel(parts, members, pick_ref, *refs):
    pair_refs = refs[: len(members)]
    base_ref, keep_ref, sum_ref = refs[len(members) :]
    here = lax.axis_index("seq") // 2
    pick = pick_ref[...]
    ones = jnp.ones((pick.shape[1], base_ref.shape[1]), jnp.bfloat16)
    taken = jnp.dot(pick, ones, preferred_element_type=jnp.float32)
    keep_ref[...] = (1.0 - taken).astype(jnp.bfloat16)
    base_ref[...] = jnp.zeros_like(base_ref)
    for index, (part, ref) in enumerate(zip(members, pair_refs)):
        rows = pair_rows(parts, ref)
        span = pl.ds(pl.multiple_of((here ^ part) * rows.shape[0], PACK), rows.shape[0])
        base_ref[span, :] = rows * keep_ref[span, :]
        for side, value in enumerate(pair_sums(parts, ref)):
            sum_ref[index, side, pl.ds(0, parts), :] = value


def bank_kernel(
    parts, members, late, share, scale, query_ref, pick_ref, ready_ref, keep_ref, sum_ref, pair_ref,
    rel_ref, bank_ref, base_ref, rel_work, bank_work, sems,
):
    group = query_ref.shape[0]
    rows = bank_ref.shape[0]
    lead = lead_rows(parts)
    me = lax.axis_index("seq")
    base_ref[...] = ready_ref[...]
    span = pl.ds(pl.multiple_of(((me // 2) ^ late) * 2 * rows, PACK), 2 * rows)
    base_ref[span, :] = pair_rows(parts, pair_ref) * keep_ref[span, :]
    fresh = []
    for side, last in enumerate(pair_sums(parts, pair_ref)):
        sums = {late: last}
        for index, part in enumerate(members):
            sums[part] = sum_ref[index, side, pl.ds(0, parts), :]
        sums = [sums[part] for part in range(parts)]
        while len(sums) > 1:
            sums = [left + right for left, right in zip(sums[::2], sums[1::2])]
        fresh.append(sums[0] * share)
        if lead > parts:
            fresh.append(jnp.zeros((lead - parts, fresh[0].shape[1]), jnp.float32))
    fresh = jnp.concatenate(fresh, axis=0).astype(jnp.bfloat16)
    placed = jnp.dot(pick_ref[...], fresh, preferred_element_type=jnp.float32)
    bank = base_ref[...] + placed.astype(jnp.bfloat16)
    base_ref[...] = bank
    bank_work[...] = base_ref[pl.ds(pl.multiple_of(me * rows, PACK), rows), :]
    copies = [pltpu.make_async_copy(bank_work, bank_ref, sems.at[group])]
    copies[0].start()
    for head in range(group):
        rel_work[head] = (nt_dot(query_ref[head], bank) * scale).astype(jnp.bfloat16)
        copies.append(pltpu.make_async_copy(rel_work.at[head], rel_ref.at[head], sems.at[head]))
        copies[-1].start()
    for copy in copies:
        copy.wait()


def per_device(count, queries, new_keys, cache_keys, window_start, owner_slot):
    tok, group, head_dim = queries.shape
    rows = cache_keys.shape[0]
    parts = count // 2
    lead = lead_rows(parts)
    assert tok == BLK and count == 1 << (count.bit_length() - 1) and count > 2
    score_scale = 1.0 / math.sqrt(head_dim)
    exp_scale = score_scale * math.log2(math.e)

    def swap(value, mask):
        return lax.ppermute(value, "seq", [(i, i ^ mask) for i in range(count)])

    def shape(rows_of, dtype):
        return jax.ShapeDtypeStruct((rows_of, head_dim), dtype)

    params = pltpu.CompilerParams(vmem_limit_bytes=(8 + parts) * MIB)
    asked = queries.transpose(1, 0, 2)
    keys = new_keys[:, 0, :]
    far = key_order(parts)
    mate = swap(asked, 1)
    pieces = {}
    for k in far:
        pieces[k] = swap(keys, 2 * k)

    cache = cache_keys[:, 0, :]
    far_cache = swap(cache, 1)
    square = jax.ShapeDtypeStruct((BLK, tok), jnp.float32)
    totals = {}
    totals[0], inside, pick, own, pieces[0] = pl.pallas_call(
        functools.partial(first_kernel, parts, exp_scale),
        out_shape=(
            square,
            jax.ShapeDtypeStruct((2, parts, tok), jnp.float32),
            jax.ShapeDtypeStruct((count * rows, 2 * lead), jnp.bfloat16),
            jax.ShapeDtypeStruct(asked.shape, jnp.bfloat16),
            jax.ShapeDtypeStruct(keys.shape, jnp.bfloat16),
        ),
        in_specs=[HBM] * 4,
        out_specs=(VMEM,) * 5,
        scratch_shapes=[
            pltpu.SMEM(window_start.shape, jnp.int32),
            pltpu.SMEM(owner_slot.shape, jnp.int32),
            pltpu.SemaphoreType.DMA((3 + group,)),
        ],
        compiler_params=params,
        name="first",
    )(*[pltpu.with_memory_space_constraint(x, pltpu.HBM) for x in (window_start, owner_slot, asked, keys)])

    *middle, tail = far
    for k in middle:
        totals[k] = pl.pallas_call(
            functools.partial(own_kernel, k, exp_scale),
            out_shape=square,
            in_specs=[VMEM] * 3,
            out_specs=VMEM,
            compiler_params=params,
        )(inside, own, pieces[k])
    members = [0, *middle]
    partial = pl.pallas_call(
        functools.partial(mate_kernel, members, exp_scale),
        out_shape=shape(padded(parts, 8), jnp.float32),
        in_specs=[VMEM] * (2 + 2 * len(members)),
        out_specs=VMEM,
        compiler_params=params,
        name="mate_step",
    )(inside, mate, *[totals[k] for k in members], *[pieces[k] for k in members])
    partial = pl.pallas_call(
        functools.partial(last_kernel, parts, tail, exp_scale),
        out_shape=shape(term_rows(parts), jnp.bfloat16),
        in_specs=[VMEM] * 5,
        out_specs=VMEM,
        scratch_shapes=[pltpu.VMEM((padded(parts, 8), head_dim), jnp.float32)],
        compiler_params=params,
        name="last",
    )(inside, partial, own, mate, pieces[tail])

    other = swap(partial, 1)
    pair = pl.pallas_call(
        pair_kernel,
        out_shape=shape(2 * (partial.shape[0] + rows), jnp.bfloat16),
        in_specs=[VMEM] * 4,
        out_specs=VMEM,
        compiler_params=params,
        name="pair",
    )(partial, other, cache, far_cache)
    pairs = [pair]
    for k in range(1, parts):
        pairs.append(swap(pair, 2 * k))

    *members, late = [0, *sum_order(parts)]
    ready, keep, sums = pl.pallas_call(
        functools.partial(prep_kernel, parts, members),
        out_shape=(
            shape(count * rows, jnp.bfloat16),
            shape(count * rows, jnp.bfloat16),
            jax.ShapeDtypeStruct((len(members), 2, padded(parts, 8), head_dim), jnp.float32),
        ),
        in_specs=[VMEM] * (1 + len(members)),
        out_specs=(VMEM,) * 3,
        compiler_params=params,
        name="prep",
    )(pick, *[pairs[part] for part in members])

    relevance, bank = pl.pallas_call(
        functools.partial(bank_kernel, parts, members, late, 1.0 / (group * WIN), score_scale),
        out_shape=(
            jax.ShapeDtypeStruct((group, tok, count * rows), jnp.bfloat16),
            jax.ShapeDtypeStruct((rows, head_dim), jnp.bfloat16),
        ),
        in_specs=[VMEM] * 6,
        out_specs=(HBM, HBM),
        scratch_shapes=[
            pltpu.VMEM((count * rows, head_dim), jnp.bfloat16),
            pltpu.VMEM((group, tok, count * rows), jnp.bfloat16),
            pltpu.VMEM((rows, head_dim), jnp.bfloat16),
            pltpu.SemaphoreType.DMA((group + 1,)),
        ],
        compiler_params=params,
        name="bank",
    )(own, pick, ready, keep, sums, pairs[late])
    return (relevance.transpose(1, 0, 2), bank[:, None, :])


def solution(mesh):
    count = mesh.shape["seq"]

    def body(*args):
        return per_device(count, *args)

    return jax.shard_map(
        body,
        mesh=mesh,
        in_specs=(P("seq", "kvh", None), P("seq", "kvh", None), P("seq", "kvh", None), P(), P()),
        out_specs=(P("seq", "kvh", None), P("seq", "kvh", None)),
        check_vma=False,
    )
```
